256 devices in a mesh: rep: 1, r: 32 (over y, z), s: 8 (over x, core).
Axes of the slice: x: 4, y: 4, z: 8, core: 2. Of those that a mesh axis runs over, the one named last changes fastest.
Arguments:
- x: bfloat16 [256, 2048, 896], P(('rep', 'r', 's'))
- dy: bfloat16 [256, 2048, 896], P(('rep', 'r', 's'))
- w_gate: bfloat16 [2, 896, 3584], P(None, 's')
- w_up: bfloat16 [2, 896, 3584], P(None, 's')
- w_down: bfloat16 [2, 3584, 896], P(None, 's')
- m_w_gate: float32 [2, 896, 3584], P(None, 's')
- m_w_up: float32 [2, 896, 3584], P(None, 's')
- m_w_down: float32 [2, 3584, 896], P(None, 's')
- v_w_gate: float32 [2, 896, 3584], P(None, 's')
- v_w_up: float32 [2, 896, 3584], P(None, 's')
- v_w_down: float32 [2, 3584, 896], P(None, 's')
Outputs:
- output 1: bfloat16 [2, 896, 3584], P('rep', 's')
- output 2: bfloat16 [2, 896, 3584], P('rep', 's')
- output 3: bfloat16 [2, 3584, 896], P('rep', 's')
- output 4: float32 [2, 896, 3584], P('rep', 's')
- output 5: float32 [2, 896, 3584], P('rep', 's')
- output 6: float32 [2, 3584, 896], P('rep', 's')
- output 7: float32 [2, 896, 3584], P('rep', 's')
- output 8: float32 [2, 896, 3584], P('rep', 's')
- output 9: float32 [2, 3584, 896], P('rep', 's')
All inputs are finite; a program needn't handle non-finite values.
Results may differ from the reference program's by a relative error of at most 0.022.
Values are sent between devices in bfloat16 or wider.
A program may use at most 768 MiB of HBM per device.

```python
import jax
import jax.numpy as jnp
from jax import lax

SEQUENCES = 256
TOKENS = 2048
D = 896
FF = 3584
LAYERS = 2
NAMES = ("w_gate", "w_up", "w_down")
SHAPES = {"w_gate": (LAYERS, D, FF), "w_up": (LAYERS, D, FF), "w_down": (LAYERS, FF, D)}


def bump(key, n, height):
    away = (jnp.arange(n, dtype=jnp.int32) - jax.random.randint(key, (), 0, n, jnp.int32)) % n
    return jnp.where(away < n // 8, height, 1.0)


def together(key, own, strength):
    shared = jax.random.normal(key, own.shape[1:], jnp.float32)
    return (own + strength * shared) * lax.rsqrt(1 + strength * strength)


def setup_inputs(seed: int = 0, part: int = 0) -> dict:
    kx, kdy, ka, kb, kz, kf, kh, kl, *keys = jax.random.split(jax.random.key(seed), 8 + 3 * len(NAMES))
    kx, kdy, ka, kb = (jax.random.fold_in(k, part) for k in (kx, kdy, ka, kb))
    kw, km, kv = (keys[i::3] for i in range(3))
    shape = (SEQUENCES, TOKENS, D)
    much_x, much_dy = jax.random.uniform(kz, (2,), jnp.float32, 0.0, 1.0)
    loud = 2.0 ** jax.random.uniform(jax.random.fold_in(kz, 1), (), jnp.float32, -1.0, 2.0)
    layers = 2.0 ** jax.random.uniform(kl, (LAYERS, 1, 1), jnp.float32, -1.0, 1.0)
    x = together(ka, jax.random.normal(kx, shape, jnp.float32), much_x) * bump(kf, D, 4.0)
    dy = together(kb, jax.random.normal(kdy, shape, jnp.float32), much_dy)
    drawn = {"x": x.astype(jnp.bfloat16), "dy": (loud * dy * (SEQUENCES * TOKENS) ** -0.5).astype(jnp.bfloat16)}
    for key, name in zip(kw, NAMES, strict=True):
        w = jax.random.normal(key, SHAPES[name], jnp.float32) * SHAPES[name][1] ** -0.5
        drawn[name] = (w * {"w_gate": 1.0, "w_up": bump(kh, FF, 4.0), "w_down": layers}[name]).astype(jnp.bfloat16)
    for key, name in zip(km, NAMES, strict=True):
        drawn[f"m_{name}"] = 0.1 * jax.random.normal(key, SHAPES[name], jnp.float32)
    for key, name in zip(kv, NAMES, strict=True):
        drawn[f"v_{name}"] = jax.random.uniform(key, SHAPES[name], jnp.float32, 0.005, 0.015)
    return drawn


def matmul(a, w):
    return jnp.dot(a, w, preferred_element_type=jnp.float32).astype(jnp.bfloat16)


def normed(h):
    wide = h.astype(jnp.float32)
    scale = lax.rsqrt(jnp.mean(wide**2, -1, keepdims=True) + 1e-6)
    return (wide * scale).astype(jnp.bfloat16)


def layer(h, w):
    a = normed(h)
    gate = jnp.dot(a, w["w_gate"], preferred_element_type=jnp.float32)
    up = jnp.dot(a, w["w_up"], preferred_element_type=jnp.float32)
    return h + matmul((jax.nn.silu(gate) * up).astype(jnp.bfloat16), w["w_down"])


def adamw(w, m, v, g):
    m = 0.9 * m + 0.1 * g
    v = 0.95 * v + 0.05 * g * g
    step = m * lax.rsqrt(v + 1e-8) + 0.1 * w
    return (w - 0.02 * step).astype(jnp.bfloat16), m, v


def clipped(gradients, sum_of_squares, count):
    factor = jnp.minimum(1.0, 0.5 * lax.rsqrt(sum_of_squares / count + 1e-30))
    return [g * factor for g in gradients]


def stack(weights, h):
    return lax.scan(lambda h, w: (layer(h, w), None), h, weights)[0]


def reference(x, dy, w_gate, w_up, w_down, m_w_gate, m_w_up, m_w_down, v_w_gate, v_w_up, v_w_down):
    weights = dict(zip(NAMES, (w_gate, w_up, w_down), strict=True))

    def take(so_far, sequence):
        h, by_y = sequence
        _, back = jax.vjp(lambda w: stack(w, h), weights)
        return jax.tree.map(lambda total, term: total + term.astype(jnp.float32), so_far, back(by_y)[0]), None

    none_yet = {name: jnp.zeros(w.shape, jnp.float32) for name, w in weights.items()}
    by_weights, _ = lax.scan(take, none_yet, (x, dy))
    gradients = [by_weights[name].astype(jnp.bfloat16).astype(jnp.float32) for name in NAMES]
    gradients = clipped(gradients, sum(jnp.sum(g * g) for g in gradients), sum(g.size for g in gradients))
    new = [
        adamw(w.astype(jnp.float32), m, v, g)
        for w, m, v, g in zip((w_gate, w_up, w_down), (m_w_gate, m_w_up, m_w_down), (v_w_gate, v_w_up, v_w_down), gradients, strict=True)
    ]
    return tuple(one[which] for which in range(3) for one in new)
```

```python
import functools

import jax
import jax.numpy as jnp
from jax import lax
from jax.experimental import pallas as pl
from jax.experimental.pallas import tpu as pltpu
from jax.sharding import PartitionSpec as P

NX, NC, NY = 4, 2, 4
S = NX * NC
U = 512
UB = U // S
LANES = 128
F32, BF16 = jnp.float32, jnp.bfloat16
MESH = pl.DeviceIdType.MESH
EPS = 1e-6


def nn(a, b):
    return lax.dot_general(a, b, (((1,), (0,)), ((), ())), preferred_element_type=F32)


def nt(a, b):
    return lax.dot_general(a, b, (((1,), (1,)), ((), ())), preferred_element_type=F32)


def tn(a, b):
    return lax.dot_general(a, b, (((0,), (0,)), ((), ())), preferred_element_type=F32)


def normed(h):
    wide = h.astype(F32)
    scale = lax.rsqrt(jnp.mean(wide * wide, -1, keepdims=True) + EPS)
    return (wide * scale).astype(BF16)


def glu_backward(g, u, dh):
    sig = jax.nn.sigmoid(g)
    silu = g * sig
    by_silu = dh * u
    return (silu * u).astype(BF16), (by_silu * (sig + silu * (1.0 - sig))).astype(BF16), (silu * dh).astype(BF16)


class Copy:
    def __init__(self, **what):
        self.what = what

    def __getattr__(self, name):
        return getattr(pltpu.make_async_remote_copy(**self.what), name)


def prep_kernel(wg, wu, og, ou, *, n_units):
    low = lax.broadcasted_iota(jnp.int32, (wg.shape[1], LANES), 1) < UB
    for w, o in ((wg, og), (wu, ou)):
        for j in range(n_units):
            for a in range(S // 2):
                first = (2 * a + j % 2) * n_units + j
                second = (2 * a + 1 - j % 2) * n_units + j
                one = w[0, :, pl.ds(first // 2 * LANES, LANES)]
                two = w[0, :, pl.ds(second // 2 * LANES, LANES)]
                o[0, j, :, pl.ds(a * LANES, LANES)] = jnp.where(low, one, two)


def prep(w_gate, w_up):
    layers, rows, ff = w_gate.shape
    n_units = ff // U
    out = jax.ShapeDtypeStruct((layers, n_units, rows, U), BF16)
    return pl.pallas_call(
        functools.partial(prep_kernel, n_units=n_units),
        grid=(layers,),
        in_specs=[pl.BlockSpec((1, rows, ff), lambda l: (l, 0, 0))] * 2,
        out_specs=[pl.BlockSpec((1, n_units, rows, U), lambda l: (l, 0, 0, 0))] * 2,
        out_shape=[out, out],
        name="prep",
    )(w_gate, w_up)


def forward_kernel(x, wg, wu, wd, h1, aT, gate, up, a, acc, *, tile):
    j = pl.program_id(0)
    tokens, d = x.shape

    @pl.when(j == 0)
    def _():
        def norm(r, _):
            rows = pl.ds(pl.multiple_of(r * tile, tile), tile)
            wide = x[rows].astype(F32)
            scale = lax.rsqrt(jnp.mean(wide * wide, -1, keepdims=True) + EPS)
            wide = wide * scale
            a[rows] = wide.astype(BF16)
            aT[:, rows] = wide.T.astype(BF16)
            acc[rows] = jnp.zeros((tile, d), F32)
            return 0

        lax.fori_loop(0, tokens // tile, norm, 0)

    swap = lax.rem(j, 2)
    w_g = wg[:, 0].reshape(d, U)
    w_u = wu[:, 0].reshape(d, U)
    w_d = jnp.concatenate([wd[2 * i + (q + swap - 2 * q * swap), 0] for i in range(S // 2) for q in range(2)], axis=0)
    for r in range(tokens // tile):
        rows = pl.ds(r * tile, tile)
        g = nn(a[rows], w_g)
        u = nn(a[rows], w_u)
        gate[0, rows] = g
        up[0, rows] = u
        hid = (g * jax.nn.sigmoid(g) * u).astype(BF16)
        acc[rows] += nn(hid, w_d)

    @pl.when(j == pl.num_programs(0) - 1)
    def _():
        def finish(r, _):
            rows = pl.ds(pl.multiple_of(r * tile, tile), tile)
            h1[rows] = x[rows] + acc[rows].astype(BF16)
            return 0

        lax.fori_loop(0, tokens // tile, finish, 0)


def forward(x, wg, wu, wd):
    tokens, d = x.shape
    n_units = wg.shape[1]
    tile = min(512, tokens)
    once = pl.Buffered(1)
    const = lambda shape: pl.BlockSpec(shape, lambda j: (0, 0), pipeline_mode=once)
    return pl.pallas_call(
        functools.partial(forward_kernel, tile=tile),
        grid=(n_units,),
        in_specs=[
            const((tokens, d)),
            pl.BlockSpec((S, 1, d // S, U), lambda j: (0, j, 0, 0)),
            pl.BlockSpec((S, 1, d // S, U), lambda j: (0, j, 0, 0)),
            pl.BlockSpec((S, 1, UB, d), lambda j: (0, j, 0, 0)),
        ],
        out_specs=[
            const((tokens, d)),
            const((d, tokens)),
            pl.BlockSpec((1, tokens, U), lambda j: (j, 0, 0)),
            pl.BlockSpec((1, tokens, U), lambda j: (j, 0, 0)),
        ],
        out_shape=[
            jax.ShapeDtypeStruct((tokens, d), BF16),
            jax.ShapeDtypeStruct((d, tokens), BF16),
            jax.ShapeDtypeStruct((n_units, tokens, U), F32),
            jax.ShapeDtypeStruct((n_units, tokens, U), F32),
        ],
        scratch_shapes=[pltpu.VMEM((tokens, d), BF16), pltpu.VMEM((tokens, d), F32)],
        compiler_params=pltpu.CompilerParams(vmem_limit_bytes=62 * 2**20),
        cost_estimate=pl.CostEstimate(flops=6 * tokens * d * U * n_units, bytes_accessed=tokens * U * n_units * 8, transcendentals=0),
        name="forward",
    )(x, wg, wu, wd)


def backward_kernel(
    h1, dy, a0T, gate0, up0, wg1, wu1, wd1, wd0,
    fgu, fd, ss,
    a1, aT, dyv, acc, hid, dgt, dup, wgv, wuv, wdv,
    ggu, gd, pgu, pd,
    sa1, ra1, sb1, rb1, sa2, ra2, sb2, rb2, res1, res2,
    sa3, ra3, sb3, rb3, sa4, ra4, sb4, rb4, q1, q2,
    zs1, zs2, zr1, zr2, gz1, gz2,
    wsem, asem, tsem,
    psend, precv, s1s, s1r, s2s, s2r, s3s, s3r, s4s, s4r, zss, zsr, gss, gsr, gls, ys, yr,
    *, tile, nz,
):
    tokens, d = dyv.shape
    units = wg1.shape[1]
    n_tiles = tokens // tile
    ngz = nz - 1
    half = ngz - ngz // 2

    s, r = lax.axis_index("s"), lax.axis_index("r")
    x, c = lax.div(s, 2), lax.rem(s, 2)
    y, z = lax.div(r, nz), lax.rem(r, nz)
    turn = lambda i, by, n: lax.rem(i + by + n, n)
    x_dev = lambda k: {"s": turn(x, k, NX) * 2 + c}
    y_dev = lambda k: {"r": turn(y, k, NY) * nz + z}
    z_dev = lambda k: {"r": y * nz + k}
    partner = {"s": x * 2 + 1 - c}

    def remote(src, dst, send, recv, dev):
        return Copy(src_ref=src, dst_ref=dst, send_sem=send, recv_sem=recv, device_id=dev, device_id_type=MESH)

    barrier = pltpu.get_barrier_semaphore()
    peers = [partner, x_dev(1), x_dev(-1), y_dev(1), y_dev(-1)]
    peers += [z_dev(turn(z, k, nz)) for k in range(1, nz)]
    for dev in peers:
        pl.semaphore_signal(barrier, inc=1, device_id=dev, device_id_type=MESH)
    pl.semaphore_wait(barrier, len(peers))


    class Ring:
        def __init__(self, me, dev, get, put, sa, ra, sb, rb, send, recv, slot_a, slot_b):
            self.me, self.get, self.put = me, get, put
            self.a = [
                remote(sa[0], ra[0], send.at[0], recv.at[slot_b, 0], dev(1)),
                remote(sa[1], ra[1], send.at[1], recv.at[slot_b, 1], dev(-1)),
            ]
            self.b = [[remote(sb[w][h], rb[w][h], send.at[2 + 2 * w + h], recv.at[slot_b, 2 + 2 * w + h], dev(1 - 2 * w)) for h in range(2)] for w in range(2)]
            self.sa, self.ra, self.sb, self.rb = sa, ra, sb, rb

        def start(self):
            far = turn(self.me, 2, 4)
            for h in range(2):
                self.sa[h][...] = self.get(far, h).astype(BF16)
                self.a[h].start()
            self.sb[0][1][...] = self.get(turn(self.me, 1, 4), 1).astype(BF16)
            self.b[0][1].start()
            self.sb[1][0][...] = self.get(turn(self.me, -1, 4), 0).astype(BF16)
            self.b[1][0].start()

        def middle(self):
            for h in range(2):
                self.a[h].wait_recv()
                near = turn(self.me, 1 - 2 * h, 4)
                self.sb[h][h][...] = (self.get(near, h) + self.ra[h][...].astype(F32)).astype(BF16)
                self.b[h][h].start()
            for h in range(2):
                self.a[h].wait_send()

        def end(self):
            for w in range(2):
                for h in range(2):
                    self.b[w][h].wait_recv()
            for h in range(2):
                self.put(h, self.get(self.me, h) + self.rb[0][h][...].astype(F32) + self.rb[1][h][...].astype(F32))
            for w in range(2):
                for h in range(2):
                    self.b[w][h].wait_send()

    def flip(u):
        j = jnp.where(u >= units, u - units, u)
        return lax.rem(j, 2)

    def ring1(u):
        g, p, a2 = lax.rem(u, 2), lax.rem(u, 3), lax.rem(u, 2)

        def get(k, h):
            return ggu[g, h, k, c].astype(F32) + pgu[p, h, k].astype(F32)

        def put(h, total):
            for k in range(NY):
                res1[k, h] = total[:, k * LANES : (k + 1) * LANES]

        return Ring(x, x_dev, get, put, [sa1.at[h] for h in range(2)], [ra1.at[a2, h] for h in range(2)],
                    [[sb1.at[a2, w, h] for h in range(2)] for w in range(2)], [[rb1.at[p, w, h] for h in range(2)] for w in range(2)], s1s.at[a2], s1r, a2, p)

    def ring2(u):
        g, p, a2 = lax.rem(u, 2), lax.rem(u, 3), lax.rem(u, 2)
        f = flip(u)
        pos = c + f - 2 * c * f

        def get(k, h):
            return gd[g, 2 * h : 2 * h + 2, pos, k].astype(F32) + pd[p, 2 * h : 2 * h + 2, k].astype(F32)

        def put(h, total):
            res2[2 * h : 2 * h + 2] = total

        return Ring(y, y_dev, get, put, [sa2.at[h] for h in range(2)], [ra2.at[a2, h] for h in range(2)],
                    [[sb2.at[a2, w, h] for h in range(2)] for w in range(2)], [[rb2.at[p, w, h] for h in range(2)] for w in range(2)], s2s.at[a2], s2r, a2, p)

    def ring3(u):
        a2 = lax.rem(u, 2)

        def get(k, h):
            return res1[k, h]

        def put(h, total):
            rows = total.shape[0] // ngz
            for k in range(ngz):
                q1[k, h] = total[k * rows : (k + 1) * rows]

        return Ring(y, y_dev, get, put, [sa3.at[h] for h in range(2)], [ra3.at[a2, h] for h in range(2)],
                    [[sb3.at[w, h] for h in range(2)] for w in range(2)], [[rb3.at[a2, w, h] for h in range(2)] for w in range(2)], s3s, s3r, a2, a2)

    cut = [slice(0, 512), slice(512, d)]

    def ring4(u):
        a2 = lax.rem(u, 2)

        def get(k, h):
            return res2[k, :, cut[h]]

        def put(h, total):
            q2[:, cut[h]] = total

        return Ring(x, x_dev, get, put, [sa4.at[:, cut[h]] for h in range(2)], [ra4.at[a2, :, cut[h]] for h in range(2)],
                    [[sb4.at[w, :, cut[h]] for h in range(2)] for w in range(2)], [[rb4.at[a2, w, :, cut[h]] for h in range(2)] for w in range(2)], s4s, s4r, a2, a2)


    def to_partner(u):
        g, p, f = lax.rem(u, 2), lax.rem(u, 3), flip(u)
        other = 1 - c
        pos = other + f - 2 * other * f
        return [
            remote(ggu.at[g, 0, :, other], pgu.at[p, 0], psend.at[0], precv.at[p, 0], partner),
            remote(ggu.at[g, 1, :, other], pgu.at[p, 1], psend.at[1], precv.at[p, 1], partner),
            remote(gd.at[g, :, pos], pd.at[p], psend.at[2], precv.at[p, 2], partner),
        ]

    def c1(u):
        copies = to_partner(u)
        copies[0].wait_recv()
        copies[1].wait_recv()
        ring1(u).start()
        copies[2].wait_recv()
        ring2(u).start()
        for copy in copies:
            copy.wait_send()

    def c2(u):
        ring1(u).middle()
        ring2(u).middle()

    def c3(u):
        ring1(u).end()
        ring3(u).start()
        ring2(u).end()
        ring4(u).start()

    def c4(u):
        ring3(u).middle()
        ring4(u).middle()

    def z_copies(u, k):
        a2 = lax.rem(u, 2)
        return [
            remote(zs1.at[k], zr1.at[a2, z], zss.at[k, 0], zsr.at[a2, z, 0], z_dev(k)),
            remote(zs2.at[k], zr2.at[a2, z], zss.at[k, 1], zsr.at[a2, z, 1], z_dev(k)),
        ]

    def c5(u):
        ring3(u).end()
        ring4(u).end()
        cols = d // ngz
        for k in range(ngz):
            zs1[k] = q1[k].astype(BF16)
            zs2[k] = q2[:, k * cols : (k + 1) * cols].astype(BF16)

            @pl.when(k != z)
            def _():
                for copy in z_copies(u, k):
                    copy.start()

    def gather_copies(u, k):
        a2 = lax.rem(u, 2)
        return [
            remote(gz1, fgu.at[u, y, z], gss.at[k, 0], gsr.at[a2, z, 0], z_dev(k)),
            remote(gz2, fd.at[u, y, z], gss.at[k, 1], gsr.at[a2, z, 1], z_dev(k)),
        ]

    def own_copies(u):
        return [pltpu.make_async_copy(gz1, fgu.at[u, y, z], gls.at[0]), pltpu.make_async_copy(gz2, fd.at[u, y, z], gls.at[1])]

    def c6(u):
        a2 = lax.rem(u, 2)

        @pl.when(z < ngz)
        def _():
            one, two = jnp.zeros(gz1.shape, F32), jnp.zeros(gz2.shape, F32)
            for k in range(nz):

                @pl.when(k != z)
                def _():
                    remote(zs1.at[0], zr1.at[a2, k], zss.at[0, 0], zsr.at[a2, k, 0], z_dev(z)).wait_recv()
                    remote(zs2.at[0], zr2.at[a2, k], zss.at[0, 1], zsr.at[a2, k, 1], z_dev(z)).wait_recv()

                own = k == z
                zone = lax.rem(z, ngz)
                one += jnp.where(own, q1[zone], zr1[a2, k].astype(F32))
                two += jnp.where(own, q2[:, pl.ds(pl.multiple_of(zone * (d // ngz), LANES), d // ngz)], zr2[a2, k].astype(F32))
            one, two = one.astype(BF16), two.astype(BF16)
            gz1[...], gz2[...] = one, two
            one, two = one.astype(F32), two.astype(F32)
            ss[...] += jnp.full(ss.shape, jnp.sum(one * one) + jnp.sum(two * two))
            for copy in own_copies(u):
                copy.start()
            for k in range(nz):

                @pl.when(k != z)
                def _():
                    for copy in gather_copies(u, k):
                        copy.start()

        for k in range(ngz):

            @pl.when(k != z)
            def _():
                for copy in z_copies(u, k):
                    copy.wait_send()

    def y_copies(u, by):
        a2 = lax.rem(u, 2)
        w = 0 if by > 0 else 1
        k = turn(y, -by, NY)
        fds = [slice(0, half), slice(half, ngz)][w]
        return [
            remote(fgu.at[u, y], fgu.at[u, y], ys.at[w, 0], yr.at[a2, w, 0], y_dev(by)),
            remote(fd.at[u, y], fd.at[u, y], ys.at[w, 1], yr.at[a2, w, 1], y_dev(by)),
        ], [
            remote(fgu.at[u, k, :, w], fgu.at[u, k, :, w], ys.at[w, 2], yr.at[a2, w, 2], y_dev(by)),
            remote(fd.at[u, k, fds], fd.at[u, k, fds], ys.at[w, 3], yr.at[a2, w, 3], y_dev(by)),
        ]

    def c7(u):
        a2 = lax.rem(u, 2)
        for k in range(ngz):

            @pl.when(k != z)
            def _():
                remote(gz1, fgu.at[u, y, k], gss.at[0, 0], gsr.at[a2, k, 0], z_dev(z)).wait_recv()
                remote(gz2, fd.at[u, y, k], gss.at[0, 1], gsr.at[a2, k, 1], z_dev(z)).wait_recv()

        @pl.when(z < ngz)
        def _():
            for copy in own_copies(u):
                copy.wait()
            for k in range(nz):

                @pl.when(k != z)
                def _():
                    for copy in gather_copies(u, k):
                        copy.wait_send()

        for by in (1, -1):
            for copy in y_copies(u, by)[0]:
                copy.start()

    def incoming(u, by, copies):
        a2 = lax.rem(u, 2)
        w = 0 if by > 0 else 1
        near, far = turn(y, -by, NY), turn(y, -2 * by, NY)
        fds = [slice(0, half), slice(half, ngz)][w]
        if copies == 0:
            return [
                remote(fgu.at[u, y], fgu.at[u, near], ys.at[w, 0], yr.at[a2, w, 0], y_dev(by)),
                remote(fd.at[u, y], fd.at[u, near], ys.at[w, 1], yr.at[a2, w, 1], y_dev(by)),
            ]
        return [
            remote(fgu.at[u, y, :, w], fgu.at[u, far, :, w], ys.at[w, 2], yr.at[a2, w, 2], y_dev(by)),
            remote(fd.at[u, y, fds], fd.at[u, far, fds], ys.at[w, 3], yr.at[a2, w, 3], y_dev(by)),
        ]

    def c8(u):
        for by in (1, -1):
            for copy in incoming(u, by, 0):
                copy.wait_recv()
            for copy in y_copies(u, by)[1]:
                copy.start()

    def c9(u):
        for by in (1, -1):
            for copy in incoming(u, by, 1):
                copy.wait_recv()
            for group in y_copies(u, by):
                for copy in group:
                    copy.wait_send()

    plan = {0: ((c5, 3), (c7, 4)), 1: ((c1, 1),), 2: ((c3, 2), (c8, 4)), 3: ((c6, 3), (c4, 2)), 4: ((c2, 1), (c9, 4))}

    def steps(t, place):
        for step, behind in plan[place]:
            u = t - behind

            @pl.when((u >= 0) & (u < 2 * units))
            def _():
                step(u)


    def weights(j, layer1):
        swap = lax.rem(j, 2)
        copies = []
        if layer1:
            copies += [pltpu.make_async_copy(wg1.at[:, j], wgv, wsem.at[0]), pltpu.make_async_copy(wu1.at[:, j], wuv, wsem.at[1])]
        wd = wd1 if layer1 else wd0
        for q in range(2):
            copies.append(pltpu.make_async_copy(wd.at[:, q, j], wdv.at[:, q + swap - 2 * q * swap], wsem.at[2 + q]))
        return copies

    def weight_gradients(t):
        g = lax.rem(t, 2)
        copies = to_partner(t)
        ggu[g, 0] = nn(aT[...], dgt[...]).astype(BF16).reshape(ggu.shape[2:])
        copies[0].start()
        steps(t, 3)
        ggu[g, 1] = nn(aT[...], dup[...]).astype(BF16).reshape(ggu.shape[2:])
        copies[1].start()
        steps(t, 4)
        gd[g] = tn(hid[...], dyv[...]).astype(BF16).reshape(gd.shape[1:])
        copies[2].start()

    first = weights(0, True)
    for copy in first:
        copy.start()
    loads = [pltpu.make_async_copy(h1, a1, asem.at[0]), pltpu.make_async_copy(dy, dyv, asem.at[1])]
    for copy in loads:
        copy.start()
    ss[...] = jnp.zeros(ss.shape, F32)
    for copy in loads:
        copy.wait()

    def norm(i, _):
        rows = pl.ds(pl.multiple_of(i * tile, tile), tile)
        wide = a1[rows].astype(F32)
        scale = lax.rsqrt(jnp.mean(wide * wide, -1, keepdims=True) + EPS)
        wide = wide * scale
        a1[rows] = wide.astype(BF16)
        aT[:, rows] = wide.T.astype(BF16)
        acc[0, rows] = jnp.zeros((tile, d), F32)
        acc[1, rows] = jnp.zeros((tile, d), F32)
        return 0

    lax.fori_loop(0, n_tiles, norm, 0)

    def both_passes(t, _):
        steps(t, 0)
        for copy in weights(t, True):
            copy.wait()
        w_g, w_u = wgv[...].reshape(d, U), wuv[...].reshape(d, U)
        w_d = wdv[...].reshape(U, d)
        for i in range(n_tiles):
            rows = pl.ds(i * tile, tile)
            av = a1[rows]
            g, u = nn(av, w_g), nn(av, w_u)
            dh = nt(dyv[rows], w_d).astype(BF16).astype(F32)
            one, by_gate, by_up = glu_backward(g, u, dh)
            hid[rows], dgt[rows], dup[rows] = one, by_gate, by_up
            acc[0, rows] += nt(by_up, w_u)
            acc[1, rows] += nt(by_gate, w_g)
            if i == min(1, n_tiles - 1):
                steps(t, 1)
        steps(t, 2)

        @pl.when(t < units - 1)
        def _():
            for copy in weights(t + 1, True):
                copy.start()

        @pl.when(t == units - 1)
        def _():
            for copy in weights(0, False):
                copy.start()

        weight_gradients(t)
        return 0

    lax.fori_loop(0, units, both_passes, 0)

    load = pltpu.make_async_copy(h1, a1, asem.at[0])
    load.start()
    loadT = pltpu.make_async_copy(a0T, aT, asem.at[1])
    loadT.start()
    load.wait()

    def cotangent(i, _):
        rows = pl.ds(pl.multiple_of(i * tile, tile), tile)
        wide = a1[rows].astype(F32)
        scale = lax.rsqrt(jnp.mean(wide * wide, -1, keepdims=True) + EPS)
        by_a = (acc[0, rows].astype(BF16).astype(F32) + acc[1, rows].astype(BF16).astype(F32)).astype(BF16).astype(F32)
        inner = jnp.sum(wide * by_a, -1, keepdims=True)
        by_h = by_a * scale - wide * (inner * (scale * scale * scale) * (1.0 / d))
        dyv[rows] = (dyv[rows].astype(F32) + by_h.astype(BF16).astype(F32)).astype(BF16)
        return 0

    lax.fori_loop(0, n_tiles, cotangent, 0)
    loadT.wait()

    def tiles(j, i, slot):
        rows = pl.ds(i * tile, tile)
        here = pl.ds(slot * tile, tile)
        return [
            pltpu.make_async_copy(gate0.at[j, rows], acc.at[0, here, 0:U], tsem.at[slot, 0]),
            pltpu.make_async_copy(up0.at[j, rows], acc.at[1, here, 0:U], tsem.at[slot, 1]),
        ]

    for i in range(n_tiles):
        for copy in tiles(0, i, i):
            copy.start()

    def backward_only(t, _):
        j = t - units
        steps(t, 0)
        for copy in weights(j, False):
            copy.wait()
        w_d = wdv[...].reshape(U, d)
        for i in range(n_tiles):
            rows = pl.ds(i * tile, tile)
            for copy in tiles(j, i, i):
                copy.wait()
            dh = nt(dyv[rows], w_d).astype(BF16).astype(F32)
            hid[rows], dgt[rows], dup[rows] = glu_backward(acc[0, rows, 0:U], acc[1, rows, 0:U], dh)
            if i == min(1, n_tiles - 1):
                steps(t, 1)
        steps(t, 2)

        @pl.when(j < units - 1)
        def _():
            for copy in weights(j + 1, False):
                copy.start()
            for i in range(n_tiles):
                for copy in tiles(j + 1, i, i):
                    copy.start()

        weight_gradients(t)
        return 0

    lax.fori_loop(units, 2 * units, backward_only, 0)

    def drain(t, _):
        for place in range(5):
            steps(t, place)
        return 0

    lax.fori_loop(2 * units, 2 * units + 5, drain, 0)


def backward(h1, dy, a0T, gate0, up0, wg1, wu1, wd1, wd0, nz):
    tokens, d = h1.shape
    units = wg1.shape[1]
    tile = min(512, tokens)
    rg, ngz = d // S, nz - 1
    rz, cz, rd = rg // ngz, d // ngz, UB // NY
    wd1, wd0 = (w.reshape(NX, NC, units, UB, d) for w in (wd1, wd0))
    vmem = lambda *shape, dtype=BF16: pltpu.VMEM(shape, dtype)
    dma = lambda *shape: pltpu.SemaphoreType.DMA(shape)
    scratch = [
        vmem(tokens, d), vmem(d, tokens), vmem(tokens, d), vmem(2, tokens, d, dtype=F32),
        vmem(tokens, U), vmem(tokens, U), vmem(tokens, U),
        vmem(S, rg, U), vmem(S, rg, U), vmem(NX, NC, UB, d),
        vmem(2, 2, NX, NC, rg, U), vmem(2, NX, NC, NY, rd, d), vmem(3, 2, NX, rg, U), vmem(3, NX, NY, rd, d),
        vmem(2, rg, U), vmem(2, 2, rg, U), vmem(2, 2, 2, rg, U), vmem(3, 2, 2, rg, U),
        vmem(2, 2, rd, d), vmem(2, 2, 2, rd, d), vmem(2, 2, 2, 2, rd, d), vmem(3, 2, 2, 2, rd, d),
        vmem(NY, 2, rg, LANES, dtype=F32), vmem(NX, rd, d, dtype=F32),
        vmem(2, rg, LANES), vmem(2, 2, rg, LANES), vmem(2, 2, rg, LANES), vmem(2, 2, 2, rg, LANES),
        vmem(rd, d), vmem(2, rd, d), vmem(2, rd, d), vmem(2, 2, rd, d),
        vmem(ngz, 2, rz, LANES, dtype=F32), vmem(rd, d, dtype=F32),
        vmem(ngz, 2, rz, LANES), vmem(ngz, rd, cz), vmem(2, nz, 2, rz, LANES), vmem(2, nz, rd, cz),
        vmem(2, rz, LANES), vmem(rd, cz),
        dma(4), dma(2), dma(max(1, tokens // tile), 2),
        dma(3), dma(3, 3), dma(2, 6), dma(3, 6), dma(2, 6), dma(3, 6), dma(6), dma(2, 6), dma(6), dma(2, 6),
        dma(ngz, 2), dma(2, nz, 2), dma(nz, 2), dma(2, nz, 2), dma(2), dma(2, 4), dma(2, 2, 4),
    ]
    anywhere = pl.BlockSpec(memory_space=pl.ANY)
    return pl.pallas_call(
        functools.partial(backward_kernel, tile=tile, nz=nz),
        in_specs=[anywhere] * 9,
        out_specs=[anywhere, anywhere, pl.BlockSpec(memory_space=pltpu.VMEM)],
        out_shape=[
            jax.ShapeDtypeStruct((2 * units, NY, ngz, 2, rz, LANES), BF16),
            jax.ShapeDtypeStruct((2 * units, NY, ngz, rd, cz), BF16),
            jax.ShapeDtypeStruct((8, LANES), F32),
        ],
        scratch_shapes=scratch,
        compiler_params=pltpu.CompilerParams(collective_id=1, has_side_effects=True, vmem_limit_bytes=67043328),
        cost_estimate=pl.CostEstimate(flops=24 * tokens * d * U * units, bytes_accessed=2**26, transcendentals=0),
        name="backward",
    )(h1, dy, a0T, gate0, up0, wg1, wu1, wd1, wd0)


def step_kernel(factor, fgu, fd, wg, mg, vg, wu, mu, vu, wd, md, vd, *out, n_units):
    ngz, rd, cz = fd.shape[2:]
    fac = factor[0, 0]

    def adamw(g, w, m, v, outs):
        g = g.astype(F32) * fac
        m = 0.9 * m + 0.1 * g
        v = 0.95 * v + 0.05 * g * g
        step = m * lax.rsqrt(v + 1e-8) + 0.1 * w.astype(F32)
        return (w.astype(F32) - 0.02 * step).astype(BF16), m, v

    rows = wg.shape[1]
    low = lax.broadcasted_iota(jnp.int32, (rows, LANES), 1) < UB
    for h, (w, m, v, outs) in enumerate(((wg, mg, vg, out[0::3]), (wu, mu, vu, out[1::3]))):
        by_unit = [jnp.concatenate([fgu[j, 0, k, h] for k in range(ngz)], axis=0).astype(F32) for j in range(n_units)]
        for i in range(n_units):
            at = pl.ds(i * LANES, LANES)
            g = jnp.where(low, by_unit[2 * i % n_units], by_unit[(2 * i + 1) % n_units])
            outs[0][0, :, at], outs[1][0, :, at], outs[2][0, :, at] = adamw(g, w[0, :, at], m[0, :, at], v[0, :, at], outs)
    for j in range(n_units):
        g = jnp.concatenate([fd[j, 0, k] for k in range(ngz)], axis=1)
        outs = out[2::3]
        outs[0][0, j, 0], outs[1][0, j, 0], outs[2][0, j, 0] = adamw(g, wd[0, j, 0], md[0, j, 0], vd[0, j, 0], outs)


def optimizer(factor, fgu, fd, weights, m, v):
    layers, rg, ff = weights[0].shape
    n_units = ff // U
    d = weights[2].shape[2]
    _, _, ngz, rd, cz = fd.shape
    rz = rg // ngz
    wide = ff // NY
    down = lambda a: a.reshape(layers, n_units, NY, rd, d)
    col = pl.BlockSpec((1, rg, wide), lambda l, a: (l, 0, a))
    row = pl.BlockSpec((1, n_units, 1, rd, d), lambda l, a: (l, 0, a, 0, 0))
    args = []
    for i in range(3):
        args += [w if i < 2 else down(w) for w in (weights[i], m[i], v[i])]
    shapes = lambda dtype: [jax.ShapeDtypeStruct((layers, rg, ff), dtype)] * 2 + [jax.ShapeDtypeStruct((layers, n_units, NY, rd, d), dtype)]
    out = pl.pallas_call(
        functools.partial(step_kernel, n_units=n_units),
        grid=(layers, NY),
        in_specs=[
            pl.BlockSpec(memory_space=pltpu.SMEM),
            pl.BlockSpec((n_units, 1, ngz, 2, rz, LANES), lambda l, a: (1 - l, a, 0, 0, 0, 0)),
            pl.BlockSpec((n_units, 1, ngz, rd, cz), lambda l, a: (1 - l, a, 0, 0, 0)),
        ]
        + [col] * 6
        + [row] * 3,
        out_specs=[col, col, row] * 3,
        out_shape=shapes(BF16) + shapes(F32) + shapes(F32),
        name="adamw",
    )(factor, fgu, fd, *args)
    return tuple(o.reshape(layers, -1, d) if i % 3 == 2 else o for i, o in enumerate(out))


def solution(mesh):
    nz = mesh.shape["r"] // NY

    def step(x, dy, *arrays):
        weights, m, v = (arrays[i : i + 3] for i in (0, 3, 6))
        layers, rg, ff = weights[0].shape
        n_units, d = ff // U, weights[2].shape[2]
        gates, ups = prep(weights[0], weights[1])
        downs = weights[2].reshape(layers, n_units, UB, d)
        whole = lambda w: lax.all_gather(w, "s", axis=0)
        wg, wu, wd = ([whole(w[l]) for l in range(layers)] for w in (gates, ups, downs))
        h1, a0T, gate0, up0 = forward(x[0], wg[0], wu[0], wd[0])
        fgu, fd, ss = backward(h1, dy[0], a0T, gate0, up0, wg[1], wu[1], wd[1], wd[0], nz)
        squares = lax.psum(ss[0, 0], ("r", "s"))
        count = lax.psum(1, "s") * sum(w.size for w in weights)
        factor = jnp.minimum(1.0, 0.5 * lax.rsqrt(squares / count + 1e-30))
        return optimizer(factor.reshape(1, 1), fgu, fd, weights, m, v)

    states, cut = P(("rep", "r", "s"), None, None), P(None, "s", None)
    return jax.shard_map(
        step,
        mesh=mesh,
        in_specs=(states, states) + (cut,) * 9,
        out_specs=(P("rep", "s", None),) * 9,
        check_vma=False,
    )
```

```python
import functools

import jax
import jax.numpy as jnp
from jax import lax
from jax.experimental import pallas as pl
from jax.experimental.pallas import tpu as pltpu
from jax.sharding import PartitionSpec as P

NX, NC, NY = 4, 2, 4
S = NX * NC
U = 512
UB = U // S
LANES = 128
TILE = 512
TWO, THREE, FOUR, SIX = 2, 3, 4, 6
BOTH = (0, 1)
F32, BF16 = jnp.float32, jnp.bfloat16
MESH = pl.DeviceIdType.MESH
EPS = 1e-6


def nn(a, b):
    return lax.dot_general(a, b, (((1,), (0,)), ((), ())), preferred_element_type=F32)


def nt(a, b):
    return lax.dot_general(a, b, (((1,), (1,)), ((), ())), preferred_element_type=F32)


def tn(a, b):
    return lax.dot_general(a, b, (((0,), (0,)), ((), ())), preferred_element_type=F32)


def scale_of(wide):
    return lax.rsqrt(jnp.mean(wide * wide, -1, keepdims=True) + EPS)


def other(bit, by):
    return bit + by - TWO * bit * by


def glu_backward(g, u, dh):
    sig = jax.nn.sigmoid(g)
    silu = g * sig
    by_silu = dh * u
    return (silu * u).astype(BF16), (by_silu * (sig + silu * (1.0 - sig))).astype(BF16), (silu * dh).astype(BF16)


class Copy:
    def __init__(self, **what):
        self.what = what

    def __getattr__(self, name):
        return getattr(pltpu.make_async_remote_copy(**self.what), name)


def start(copies):
    for copy in copies:
        copy.start()


def arrived(copies):
    for copy in copies:
        copy.wait_recv()


def sent(copies):
    for copy in copies:
        copy.wait_send()


def done(copies):
    for copy in copies:
        copy.wait()


def prep_kernel(wg, wu, wd, wgu, wdn, block, sem, *, units):
    layers, rows, _ = wg.shape
    s = lax.axis_index("s")
    x, c = lax.div(s, NC), lax.rem(s, NC)
    low = lax.broadcasted_iota(jnp.int32, (rows, LANES), 1) < UB
    copies = []
    for l in range(layers):
        for j in range(units):
            copies.append(pltpu.make_async_copy(wd.at[l, j], wdn.at[l * units + j, x, c], sem.at[1, l, j]))
    start(copies)
    for l in range(layers):
        for j in range(units):
            for h, w in enumerate((wg, wu)):
                for a in range(NX):
                    swap = j % TWO
                    first = (TWO * a + swap) * units + j
                    second = (TWO * a + 1 - swap) * units + j
                    one = w[l, :, pl.ds(first // TWO * LANES, LANES)]
                    two = w[l, :, pl.ds(second // TWO * LANES, LANES)]
                    block[l, j, h, :, pl.ds(a * LANES, LANES)] = jnp.where(low, one, two)
            copy = pltpu.make_async_copy(block.at[l, j], wgu.at[l * units + j, :, x, c], sem.at[0, l, j])
            copy.start()
            copies.append(copy)
    done(copies)


def prep(w_gate, w_up, w_down):
    layers, rows, ff = w_gate.shape
    units, d = ff // U, w_down.shape[-1]
    anywhere = pl.BlockSpec(memory_space=pl.ANY)
    return pl.pallas_call(
        functools.partial(prep_kernel, units=units),
        in_specs=[pl.BlockSpec(memory_space=pltpu.VMEM)] * 3,
        out_specs=[anywhere] * 2,
        out_shape=[jax.ShapeDtypeStruct((layers * units, 2, NX, NC, rows, U), BF16), jax.ShapeDtypeStruct((layers * units, NX, NC, UB, d), BF16)],
        scratch_shapes=[pltpu.VMEM((layers, units, 2, rows, U), BF16), pltpu.SemaphoreType.DMA((2, layers, units))],
        name="prep",
    )(w_gate, w_up, w_down.reshape(layers, units, UB, d))


def layers_kernel(
    x0, dy, wgu_in, wdn_in,
    wgu, wdn, h1, a0T, gate0, up0, fgu, fd,
    squares,
    a1, aT, dyv, acc, hid, dgt, dup, wv, wdv, upt,
    ggu, gd, pgu, pd,
    sa1, ra1, sb1, rb1, sa2, ra2, sb2, rb2, res1, res2,
    sa3, ra3, sb3, rb3, sa4, ra4, sb4, rb4, q1, q2,
    zs1, zs2, zr1, zr2, gz1, gz2, ss, sr,
    wsem, asem, tsem,
    psend, precv, s1s, s1r, s2s, s2r, s3s, s3r, s4s, s4r, zss, zsr, gss, gsr, gls, ys, yr, qss, qsr,
    xas, xar, xbs, xbr, yas, yar, ybs, ybr, dds, ddr,
    *, tile, nz,
):
    tokens, d = dyv.shape
    total_units = wgu.shape[0]
    units = total_units // TWO
    n_tiles = tokens // tile
    ngz = nz - 1
    half = ngz - ngz // TWO

    s, r = lax.axis_index("s"), lax.axis_index("r")
    x, c = lax.div(s, NC), lax.rem(s, NC)
    y, z = lax.div(r, nz), lax.rem(r, nz)
    turn = lambda i, by, n: lax.rem(i + by + n, n)
    x_dev = lambda k: {"s": turn(x, k, NX) * NC + c}
    y_dev = lambda k: {"r": turn(y, k, NY) * nz + z}
    z_dev = lambda k: {"r": y * nz + k}
    partner = {"s": x * NC + 1 - c}
    ways = tuple(enumerate((1, -1)))

    def remote(src, dst, send, recv, dev):
        return Copy(src_ref=src, dst_ref=dst, send_sem=send, recv_sem=recv, device_id=dev, device_id_type=MESH)

    def when(condition, do):
        pl.when(condition)(do)

    barrier = pltpu.get_barrier_semaphore()
    peers = [partner] + [dev(k) for dev in (x_dev, y_dev) for k in range(1, NX)]
    peers += [z_dev(turn(z, k, nz)) for k in range(1, nz)]
    for dev in peers:
        pl.semaphore_signal(barrier, inc=1, device_id=dev, device_id_type=MESH)
    pl.semaphore_wait(barrier, len(peers))

    def cols(k):
        return pl.ds(pl.multiple_of(k * LANES, LANES), LANES)

    def piece(v, k, q):
        return wgu.at[v, :, k, c, :, cols(q)]

    def x_first(v):
        a2 = lax.rem(v, TWO)
        for w, by in ways:
            out = [(piece(v, x, y), 0), (wdn.at[v, x, c], 1)]
            yield by, [remote(ref, ref, xas.at[a2, w, i], xar.at[a2, w, i], x_dev(by)) for ref, i in out]

    def x_second(v):
        a2 = lax.rem(v, TWO)
        for w, by in ways:
            k = turn(x, -by, NX)
            out = [(wgu.at[v, w, k, c, :, cols(y)], 0), (wdn.at[v, k, c, pl.ds(w * (UB // TWO), UB // TWO)], 1)]
            yield by, [remote(ref, ref, xbs.at[a2, w, i], xbr.at[a2, w, i], x_dev(by)) for ref, i in out]

    def y_first(v, which):
        a2 = lax.rem(v, TWO)
        for w, by in ways:
            out = [(piece(v, turn(x, i, NX), y), i) for i in which]
            yield by, [remote(ref, ref, yas.at[a2, w, i], yar.at[a2, w, i], y_dev(by)) for ref, i in out]

    def y_second(v, which):
        a2 = lax.rem(v, TWO)
        for w, by in ways:
            out = [(wgu.at[v, w, turn(x, i, NX), c, :, cols(turn(y, -by, NY))], i) for i in which]
            yield by, [remote(ref, ref, ybs.at[a2, w, i], ybr.at[a2, w, i], y_dev(by)) for ref, i in out]

    def across(v):
        a2 = lax.rem(v, TWO)
        out = [(wgu.at[v, :, :, c], 0), (wdn.at[v, :, c], 1)]
        return [remote(ref, ref, dds.at[a2, i], ddr.at[a2, i], partner) for ref, i in out]

    def every(groups):
        return [copy for _, group in groups for copy in group]

    near, far = (1, NX - 1), (TWO,)

    def g1(v):
        start(every(x_first(v)))

    def g2(v):
        arrived(every(x_first(v)))
        start(every(x_second(v)))
        start(every(y_first(v, near)))

    def g3(v):
        arrived(every(x_second(v)))
        start(every(y_first(v, far)))
        arrived(every(y_first(v, near)))
        start(every(y_second(v, near)))
        sent(every(x_first(v)))

    def g4(v):
        arrived(every(y_first(v, far)))
        start(every(y_second(v, far)))
        arrived(every(y_second(v, near)))
        sent(every(x_second(v)))
        sent(every(y_first(v, near)))

    def g5(v):
        arrived(every(y_second(v, far)))
        start(across(v))
        sent(every(y_first(v, far)))
        sent(every(y_second(v, near)))

    def g6(v):
        arrived(across(v))
        sent(across(v))
        sent(every(y_second(v, far)))
        start(weights(v))

    stages = (g1, g2, g3, g4, g5, g6)

    def gather(t, *numbers):
        for number in numbers:
            v = t - (number - 1)
            when((v >= 0) & (v < total_units), functools.partial(stages[number - 1], v))

    def weights(v, down_only=False):
        slot, unit = lax.rem(v, TWO), lax.rem(v, total_units)
        swap = lax.rem(lax.rem(unit, units), TWO)
        copies = [] if down_only else [pltpu.make_async_copy(wgu.at[unit, h], wv.at[slot, h], wsem.at[slot, h]) for h in BOTH]
        for q in BOTH:
            copies.append(pltpu.make_async_copy(wdn.at[unit, :, q], wdv.at[slot, :, other(q, swap)], wsem.at[slot, TWO + q]))
        return copies

    class Ring:
        def __init__(self, me, dev, get, put, buffers, send, recv):
            self.me, self.get, self.put = me, get, put
            self.sa, self.ra, self.sb, self.rb = buffers
            self.a = [remote(self.sa(w), self.ra(w), send.at[w], recv.at[w], dev(by)) for w, by in ways]
            at = lambda w, h: TWO + TWO * w + h
            self.b = [[remote(self.sb(w, h), self.rb(w, h), send.at[at(w, h)], recv.at[at(w, h)], dev(by)) for h in BOTH] for w, by in ways]

        def start(self):
            for h in BOTH:
                self.sa(h)[...] = self.get(turn(self.me, TWO, FOUR), h).astype(BF16)
                self.a[h].start()
            for w, by in ways:
                self.sb(w, 1 - w)[...] = self.get(turn(self.me, by, FOUR), 1 - w).astype(BF16)
                self.b[w][1 - w].start()

        def middle(self):
            for h, by in ways:
                self.a[h].wait_recv()
                self.sb(h, h)[...] = (self.get(turn(self.me, by, FOUR), h) + self.ra(h)[...].astype(F32)).astype(BF16)
                self.b[h][h].start()
            sent(self.a)

        def end(self):
            for w in BOTH:
                arrived(self.b[w])
            for h in BOTH:
                self.put(h, self.get(self.me, h) + self.rb(0, h)[...].astype(F32) + self.rb(1, h)[...].astype(F32))
            for w in BOTH:
                sent(self.b[w])

    def slots(u):
        return lax.rem(u, TWO), lax.rem(u, THREE), lax.rem(lax.rem(u, units), TWO)

    def ring1(u):
        a2, p, _ = slots(u)

        def get(k, h):
            return ggu[a2, h, k, c].astype(F32) + pgu[p, h, k].astype(F32)

        def put(h, total):
            for k in range(NY):
                res1[k, h] = total[:, k * LANES : (k + 1) * LANES]

        buffers = lambda h: sa1.at[h], lambda h: ra1.at[a2, h], lambda w, h: sb1.at[a2, w, h], lambda w, h: rb1.at[p, w, h]
        return Ring(x, x_dev, get, put, buffers, s1s.at[a2], s1r.at[p])

    def ring2(u):
        a2, p, swap = slots(u)
        pos = other(c, swap)

        def get(k, h):
            return gd[a2, pl.ds(TWO * h, TWO), pos, k].astype(F32) + pd[p, pl.ds(TWO * h, TWO), k].astype(F32)

        def put(h, total):
            res2[pl.ds(TWO * h, TWO)] = total

        buffers = lambda h: sa2.at[h], lambda h: ra2.at[a2, h], lambda w, h: sb2.at[a2, w, h], lambda w, h: rb2.at[p, w, h]
        return Ring(y, y_dev, get, put, buffers, s2s.at[a2], s2r.at[p])

    def ring3(u):
        a2, _, _ = slots(u)

        def get(k, h):
            return res1[k, h]

        def put(h, total):
            rows = total.shape[0] // ngz
            for k in range(ngz):
                q1[k, h] = total[k * rows : (k + 1) * rows]

        buffers = lambda h: sa3.at[h], lambda h: ra3.at[a2, h], lambda w, h: sb3.at[w, h], lambda w, h: rb3.at[a2, w, h]
        return Ring(y, y_dev, get, put, buffers, s3s, s3r.at[a2])

    cut = [pl.ds(0, U), pl.ds(U, d - U)]

    def ring4(u):
        a2, _, _ = slots(u)

        def get(k, h):
            return res2[k, :, cut[h]]

        def put(h, total):
            q2[:, cut[h]] = total

        buffers = lambda h: sa4.at[:, cut[h]], lambda h: ra4.at[a2, :, cut[h]], lambda w, h: sb4.at[w, :, cut[h]], lambda w, h: rb4.at[a2, w, :, cut[h]]
        return Ring(x, x_dev, get, put, buffers, s4s, s4r.at[a2])

    def to_partner(u):
        a2, p, swap = slots(u)
        ends = [(ggu.at[a2, h, :, 1 - c], pgu.at[p, h]) for h in BOTH] + [(gd.at[a2, :, other(1 - c, swap)], pd.at[p])]
        return [remote(src, dst, psend.at[i], precv.at[p, i], partner) for i, (src, dst) in enumerate(ends)]

    def c1(u):
        copies = to_partner(u)
        arrived(copies[:TWO])
        ring1(u).start()
        arrived(copies[TWO:])
        ring2(u).start()
        sent(copies)

    def c2(u):
        ring1(u).middle()
        ring2(u).middle()

    def c3(u):
        ring1(u).end()
        ring3(u).start()
        ring2(u).end()
        ring4(u).start()

    def c4(u):
        ring3(u).middle()
        ring4(u).middle()

    def others(n, do):
        for k in range(n):
            when(k != z, functools.partial(do, k))

    def z_copies(u, k, sender=None):
        a2 = lax.rem(u, TWO)
        sender = z if sender is None else sender
        ends = (zs1.at[k], zr1.at[a2, sender]), (zs2.at[k], zr2.at[a2, sender])
        return [remote(src, dst, zss.at[k, i], zsr.at[a2, sender, i], z_dev(k)) for i, (src, dst) in enumerate(ends)]

    def c5(u):
        ring3(u).end()
        ring4(u).end()
        width = d // ngz
        for k in range(ngz):
            zs1[k] = q1[k].astype(BF16)
            zs2[k] = q2[:, pl.ds(k * width, width)].astype(BF16)
        others(ngz, lambda k: start(z_copies(u, k)))

    def gather_copies(u, k, sender=None):
        a2 = lax.rem(u, TWO)
        sender = z if sender is None else sender
        ends = (gz1, fgu.at[u, y, sender]), (gz2, fd.at[u, y, sender])
        return [remote(src, dst, gss.at[k, i], gsr.at[a2, sender, i], z_dev(k)) for i, (src, dst) in enumerate(ends)]

    def own_copies(u):
        return [pltpu.make_async_copy(gz1, fgu.at[u, y, z], gls.at[0]), pltpu.make_async_copy(gz2, fd.at[u, y, z], gls.at[1])]

    def c6(u):
        a2 = lax.rem(u, TWO)

        def sums():
            others(nz, lambda k: arrived(z_copies(u, 0, k)))
            zone, width = lax.rem(z, ngz), d // ngz
            one, two = q1[zone], q2[:, pl.ds(pl.multiple_of(zone * width, LANES), width)]
            for k in range(nz):
                one += jnp.where(k == z, 0.0, zr1[a2, k].astype(F32))
                two += jnp.where(k == z, 0.0, zr2[a2, k].astype(F32))
            one, two = one.astype(BF16), two.astype(BF16)
            gz1[...], gz2[...] = one, two
            one, two = one.astype(F32), two.astype(F32)
            ss[...] += jnp.full(ss.shape, jnp.sum(one * one) + jnp.sum(two * two))
            start(own_copies(u))
            others(nz, lambda k: start(gather_copies(u, k)))

        when(z < ngz, sums)
        others(ngz, lambda k: sent(z_copies(u, k)))

    def y_copies(u, by, second, sender_y=None):
        a2 = lax.rem(u, TWO)
        w = 0 if by > 0 else 1
        if not second:
            ends = fgu.at[u, y], fd.at[u, y]
        else:
            k = turn(y, -by, NY)
            ends = fgu.at[u, k, :, w], fd.at[u, k, (pl.ds(0, half), pl.ds(half, ngz - half))[w]]
        return [remote(ref, ref, ys.at[w, second, i], yr.at[a2, w, second, i], y_dev(by)) for i, ref in enumerate(ends)]

    def c7(u):
        others(ngz, lambda k: arrived(gather_copies(u, 0, k)))

        def mine():
            done(own_copies(u))
            others(nz, lambda k: sent(gather_copies(u, k)))

        when(z < ngz, mine)
        for _, by in ways:
            start(y_copies(u, by, 0))

    def c8(u):
        for _, by in ways:
            arrived(y_copies(u, by, 0))
            start(y_copies(u, by, 1))

    def c9(u):
        for _, by in ways:
            arrived(y_copies(u, by, 1))
            sent(y_copies(u, by, 0))
            sent(y_copies(u, by, 1))

    plan = {0: ((c5, THREE), (c7, FOUR)), 1: ((c1, 1),), 2: ((c3, TWO), (c8, FOUR)), 3: ((c6, THREE), (c4, TWO)), 4: ((c2, 1), (c9, FOUR))}

    def steps(t, place):
        for step, behind in plan[place]:
            u = t - behind
            when((u >= 0) & (u < total_units), functools.partial(step, u))

    def rows_of(i):
        return pl.ds(pl.multiple_of(i * tile, tile), tile)

    def weight_gradients(t):
        a2 = lax.rem(t, TWO)
        copies = to_partner(t)
        for h, by in enumerate((dgt, dup)):
            ggu[a2, h] = nn(aT[...], by[...]).astype(BF16).reshape(ggu.shape[TWO:])
            copies[h].start()
            steps(t, THREE + h)
        gd[a2] = tn(hid[...], dyv[...]).astype(BF16).reshape(gd.shape[1:])
        copies[TWO].start()

    load = pltpu.make_async_copy(x0, dyv, asem.at[0])
    load.start()
    gather(0, 1)
    ss[...] = jnp.zeros(ss.shape, F32)
    load.wait()
    keep = pltpu.make_async_copy(aT, a0T, asem.at[1])

    def norm(i, _):
        rows = rows_of(i)
        wide = dyv[rows].astype(F32)
        wide = wide * scale_of(wide)
        a1[rows] = wide.astype(BF16)
        aT[:, rows] = wide.T.astype(BF16)
        acc[0, rows] = jnp.zeros((tile, d), F32)
        return 0

    lax.fori_loop(0, n_tiles, norm, 0)
    keep.start()

    def fill(t, _):
        gather(t, 6, 5, 4, 3, 2, 1)
        return 0

    lax.fori_loop(1, SIX, fill, 0)

    def out_tile(j, i):
        slot = i % TWO
        at = pl.ds(slot * tile, tile)
        return [pltpu.make_async_copy(acc.at[1, at, pl.ds(0, U)], gate0.at[j, pl.ds(i * tile, tile)], tsem.at[slot, 0]),
                pltpu.make_async_copy(upt.at[at], up0.at[j, pl.ds(i * tile, tile)], tsem.at[slot, 1])]

    def forward(j, _):
        t = j + SIX
        slot = lax.rem(j, TWO)
        gather(t, 6)
        done(weights(j))
        w_g, w_u, w_d = wv[slot, 0].reshape(d, U), wv[slot, 1].reshape(d, U), wdv[slot].reshape(U, d)
        for i in range(n_tiles):
            rows = pl.ds(i * tile, tile)
            at = pl.ds(i % TWO * tile, tile)
            if i < TWO:
                when(j > 0, lambda: done(out_tile(j, i)))
            else:
                done(out_tile(j, i))
            g, u = nn(a1[rows], w_g), nn(a1[rows], w_u)
            acc[1, at, pl.ds(0, U)], upt[at] = g, u
            start(out_tile(j, i))
            acc[0, rows] += nn((g * jax.nn.sigmoid(g) * u).astype(BF16), w_d)
            gather(t, *((5,), (4, 3), (2, 1), ())[i])
        return 0

    lax.fori_loop(0, units, forward, 0)
    for i in range(min(TWO, n_tiles)):
        done(out_tile(0, i))
    keep.wait()

    def between(i, _):
        rows = rows_of(i)
        h = dyv[rows] + acc[0, rows].astype(BF16)
        hid[rows], dgt[rows, cut_low] = h[:, :U], h[:, U:]
        pltpu.make_async_copy(dy.at[rows], dyv.at[rows], asem.at[0]).start()
        wide = h.astype(F32)
        wide = wide * scale_of(wide)
        a1[rows] = wide.astype(BF16)
        aT[:, rows] = wide.T.astype(BF16)
        for h in BOTH:
            acc[h, rows] = jnp.zeros((tile, d), F32)
        return 0

    cut_low = pl.ds(0, d - U)
    lax.fori_loop(0, n_tiles, between, 0)
    keep = [pltpu.make_async_copy(hid, h1.at[:, cut[0]], asem.at[1]), pltpu.make_async_copy(dgt.at[:, cut_low], h1.at[:, cut[1]], asem.at[TWO])]
    start(keep)
    pltpu.make_async_copy(dy, dyv, asem.at[0]).wait()
    done(keep)

    def both_passes(t, _):
        v = t + units
        slot = lax.rem(v, TWO)
        steps(t, 0)
        gather(v + SIX, 6, 5, 4)
        when(t == units - 1, lambda: start(weights(total_units, True)))
        done(weights(v))
        w_g, w_u, w_d = wv[slot, 0].reshape(d, U), wv[slot, 1].reshape(d, U), wdv[slot].reshape(U, d)
        for i in range(n_tiles):
            rows = pl.ds(i * tile, tile)
            g, u = nn(a1[rows], w_g), nn(a1[rows], w_u)
            dh = nt(dyv[rows], w_d).astype(BF16).astype(F32)
            hid[rows], by_gate, by_up = glu_backward(g, u, dh)
            dgt[rows], dup[rows] = by_gate, by_up
            acc[0, rows] += nt(by_up, w_u)
            acc[1, rows] += nt(by_gate, w_g)
            if i == min(1, n_tiles - 1):
                steps(t, 1)
                gather(v + SIX, 3, 2, 1)
        steps(t, TWO)
        weight_gradients(t)
        return 0

    lax.fori_loop(0, units, both_passes, 0)

    loads = [pltpu.make_async_copy(h1, a1, asem.at[0]), pltpu.make_async_copy(a0T, aT, asem.at[1])]
    start(loads)
    loads[0].wait()

    def cotangent(i, _):
        rows = rows_of(i)
        wide = a1[rows].astype(F32)
        scale = scale_of(wide)
        by_a = (acc[0, rows].astype(BF16).astype(F32) + acc[1, rows].astype(BF16).astype(F32)).astype(BF16).astype(F32)
        inner = jnp.sum(wide * by_a, -1, keepdims=True)
        by_h = by_a * scale - wide * (inner * (scale * scale * scale) * (1.0 / d))
        dyv[rows] = (dyv[rows].astype(F32) + by_h.astype(BF16).astype(F32)).astype(BF16)
        return 0

    lax.fori_loop(0, n_tiles, cotangent, 0)
    loads[1].wait()

    def in_tile(j, i):
        rows = pl.ds(i * tile, tile)
        ends = (gate0, 0), (up0, 1)
        return [pltpu.make_async_copy(src.at[j, rows], acc.at[h, rows, pl.ds(0, U)], tsem.at[TWO + i, h]) for src, h in ends]

    for i in range(n_tiles):
        start(in_tile(0, i))

    def backward_only(t, _):
        j = t - units
        v = t + units
        slot = lax.rem(v, TWO)
        steps(t, 0)
        when(j < units - 1, lambda: start(weights(v + 1, True)))
        done(weights(v, True))
        w_d = wdv[slot].reshape(U, d)
        for i in range(n_tiles):
            rows = pl.ds(i * tile, tile)
            done(in_tile(j, i))
            dh = nt(dyv[rows], w_d).astype(BF16).astype(F32)
            hid[rows], dgt[rows], dup[rows] = glu_backward(acc[0, rows, pl.ds(0, U)], acc[1, rows, pl.ds(0, U)], dh)
            if i == min(1, n_tiles - 1):
                steps(t, 1)
        steps(t, TWO)

        def ahead():
            for i in range(n_tiles):
                start(in_tile(j + 1, i))

        when(j < units - 1, ahead)
        weight_gradients(t)
        return 0

    lax.fori_loop(units, total_units, backward_only, 0)

    for t in range(THREE):
        for place in plan:
            steps(total_units + t, place)

    def exchange(number, devs):
        copies = [remote(ss, sr.at[number, i], qss.at[number, i], qsr.at[number, i], dev) for i, dev in enumerate(devs)]
        start(copies)

        def finish():
            arrived(copies)
            sent(copies)
            total = ss[...]
            for i in range(len(devs)):
                total += sr[number, i]
            ss[...] = total

        return finish

    last = total_units - 1
    finish = exchange(0, [z_dev(turn(z, k, nz)) for k in range(1, nz)])
    finish()
    finish = exchange(1, [y_dev(k) for k in range(1, NY)])
    c7(last)
    finish()
    finish = exchange(TWO, [x_dev(k) for k in range(1, NX)])
    c8(last)
    finish()
    finish = exchange(THREE, [partner])
    c9(last)
    finish()
    squares[...] = ss[...]


def layers(x, dy, wgu, wdn, nz):
    tokens, d = x.shape
    units = wgu.shape[0] // TWO
    tile = TILE
    n_tiles = tokens // tile
    rg, ngz = d // S, nz - 1
    rz, cz, rd = rg // ngz, d // ngz, UB // NY
    vmem = lambda *shape, dtype=BF16: pltpu.VMEM(shape, dtype)
    slots = lambda *shape: [vmem(*lead, *shape) for lead in ((TWO,), (TWO, TWO), (TWO, TWO, TWO), (THREE, TWO, TWO))]
    small = lambda *shape: [vmem(*lead, *shape) for lead in ((TWO,), (TWO, TWO), (TWO, TWO), (TWO, TWO, TWO))]
    narrow = lambda *shape: [vmem(*lead, *shape) for lead in ((), (TWO,), (TWO,), (TWO, TWO))]
    dma = lambda *shape: pltpu.SemaphoreType.DMA(shape)
    scratch = [
        vmem(tokens, d), vmem(d, tokens), vmem(tokens, d), vmem(TWO, tokens, d, dtype=F32),
        vmem(tokens, U), vmem(tokens, U), vmem(tokens, U),
        vmem(TWO, TWO, NX, NC, rg, U), vmem(TWO, NX, NC, UB, d), vmem(min(TWO, n_tiles) * tile, U, dtype=F32),
        vmem(TWO, TWO, NX, NC, rg, U), vmem(TWO, NX, NC, NY, rd, d), vmem(THREE, TWO, NX, rg, U), vmem(THREE, NX, NY, rd, d),
        *slots(rg, U), *slots(TWO, rd, d),
        vmem(NY, TWO, rg, LANES, dtype=F32), vmem(NX, rd, d, dtype=F32),
        *small(rg, LANES), *narrow(rd, d),
        vmem(ngz, TWO, rz, LANES, dtype=F32), vmem(rd, d, dtype=F32),
        vmem(ngz, TWO, rz, LANES), vmem(ngz, rd, cz), vmem(TWO, nz, TWO, rz, LANES), vmem(TWO, nz, rd, cz),
        vmem(TWO, rz, LANES), vmem(rd, cz), vmem(S, LANES, dtype=F32), vmem(FOUR, max(nz, NX), S, LANES, dtype=F32),
        dma(TWO, FOUR), dma(THREE), dma(TWO + n_tiles, TWO),
        dma(THREE), dma(THREE, THREE), dma(TWO, SIX), dma(THREE, SIX), dma(TWO, SIX), dma(THREE, SIX), dma(SIX), dma(TWO, SIX), dma(SIX), dma(TWO, SIX),
        dma(ngz, TWO), dma(TWO, nz, TWO), dma(nz, TWO), dma(TWO, nz, TWO), dma(TWO), dma(TWO, TWO, TWO), dma(TWO, TWO, TWO, TWO), dma(FOUR, nz), dma(FOUR, nz),
        dma(TWO, TWO, TWO), dma(TWO, TWO, TWO), dma(TWO, TWO, TWO), dma(TWO, TWO, TWO), dma(TWO, TWO, NX), dma(TWO, TWO, NX), dma(TWO, TWO, NX), dma(TWO, TWO, NX), dma(TWO, TWO), dma(TWO, TWO),
    ]
    anywhere = pl.BlockSpec(memory_space=pl.ANY)
    array = jax.ShapeDtypeStruct
    return pl.pallas_call(
        functools.partial(layers_kernel, tile=tile, nz=nz),
        in_specs=[anywhere] * FOUR,
        out_specs=[anywhere] * S + [pl.BlockSpec(memory_space=pltpu.VMEM)],
        out_shape=[
            array(wgu.shape, BF16),
            array(wdn.shape, BF16),
            array((tokens, d), BF16),
            array((d, tokens), BF16),
            array((units, tokens, U), F32),
            array((units, tokens, U), F32),
            array((TWO * units, NY, ngz, TWO, rz, LANES), BF16),
            array((TWO * units, NY, ngz, rd, cz), BF16),
            array((S, LANES), F32),
        ],
        scratch_shapes=scratch,
        input_output_aliases={TWO: 0, THREE: 1},
        compiler_params=pltpu.CompilerParams(collective_id=1, has_side_effects=True, vmem_limit_bytes=67043328),
        cost_estimate=pl.CostEstimate(flops=15 * TWO * tokens * d * U * units, bytes_accessed=2**28, transcendentals=0),
        name="layers",
    )(x, dy, wgu, wdn)[SIX:]


def step_kernel(squares, fgu, fd, wg, mg, vg, wu, mu, vu, wd, md, vd, *out, n_units, count):
    ngz, rd, cz = fd.shape[2:]
    fac = jnp.minimum(1.0, 0.5 * lax.rsqrt(squares[0:1] / count + 1e-30))[:, 0:1]

    def adamw(g, w, m, v):
        g = g.astype(F32) * fac
        m = 0.9 * m + 0.1 * g
        v = 0.95 * v + 0.05 * g * g
        step = m * lax.rsqrt(v + 1e-8) + 0.1 * w.astype(F32)
        return (w.astype(F32) - 0.02 * step).astype(BF16), m, v

    rows = wg.shape[1]
    low = lax.broadcasted_iota(jnp.int32, (rows, LANES), 1) < UB
    for h, (w, m, v, outs) in enumerate(((wg, mg, vg, out[0::THREE]), (wu, mu, vu, out[1::THREE]))):
        by_unit = [jnp.concatenate([fgu[j, 0, k, h] for k in range(ngz)], axis=0).astype(F32) for j in range(n_units)]
        for i in range(n_units):
            at = pl.ds(i * LANES, LANES)
            g = jnp.where(low, by_unit[TWO * i % n_units], by_unit[(TWO * i + 1) % n_units])
            outs[0][0, :, at], outs[1][0, :, at], outs[2][0, :, at] = adamw(g, w[0, :, at], m[0, :, at], v[0, :, at])
    outs = out[TWO::THREE]
    for j in range(n_units):
        g = jnp.concatenate([fd[j, 0, k] for k in range(ngz)], axis=1)
        outs[0][0, j, 0], outs[1][0, j, 0], outs[2][0, j, 0] = adamw(g, wd[0, j, 0], md[0, j, 0], vd[0, j, 0])


def optimizer(squares, fgu, fd, weights, m, v):
    layers, rg, ff = weights[0].shape
    n_units = ff // U
    d = weights[2].shape[2]
    _, _, ngz, rd, cz = fd.shape
    rz = rg // ngz
    wide = ff // NY
    down = lambda a: a.reshape(layers, n_units, NY, rd, d)
    col = pl.BlockSpec((1, rg, wide), lambda l, a: (l, 0, a))
    row = pl.BlockSpec((1, n_units, 1, rd, d), lambda l, a: (l, 0, a, 0, 0))
    args = []
    for i in range(3):
        args += [w if i < 2 else down(w) for w in (weights[i], m[i], v[i])]
    shapes = lambda dtype: [jax.ShapeDtypeStruct((layers, rg, ff), dtype)] * 2 + [jax.ShapeDtypeStruct((layers, n_units, NY, rd, d), dtype)]
    out = pl.pallas_call(
        functools.partial(step_kernel, n_units=n_units, count=S * sum(w.size for w in weights)),
        grid=(layers, NY),
        in_specs=[
            pl.BlockSpec((S, LANES), lambda l, a: (0, 0)),
            pl.BlockSpec((n_units, 1, ngz, 2, rz, LANES), lambda l, a: (1 - l, a, 0, 0, 0, 0)),
            pl.BlockSpec((n_units, 1, ngz, rd, cz), lambda l, a: (1 - l, a, 0, 0, 0)),
        ]
        + [col] * 6
        + [row] * 3,
        out_specs=[col, col, row] * 3,
        out_shape=shapes(BF16) + shapes(F32) + shapes(F32),
        name="adamw",
    )(squares, fgu, fd, *args)
    return tuple(o.reshape(layers, -1, d) if i % 3 == 2 else o for i, o in enumerate(out))


def solution(mesh):
    nz = mesh.shape["r"] // NY

    def step(x, dy, *arrays):
        weights, m, v = (arrays[i : i + THREE] for i in (0, THREE, SIX))
        fgu, fd, squares = layers(x[0], dy[0], *prep(*weights), nz)
        return optimizer(squares, fgu, fd, weights, m, v)

    states, cut = P(("rep", "r", "s"), None, None), P(None, "s", None)
    return jax.shard_map(
        step,
        mesh=mesh,
        in_specs=(states, states) + (cut,) * 9,
        out_specs=(P("rep", "s", None),) * 9,
        check_vma=False,
    )
```

```python
import functools

import jax
import jax.numpy as jnp
from jax import lax
from jax.experimental import pallas as pl
from jax.experimental.pallas import tpu as pltpu
from jax.sharding import PartitionSpec as P

NX, NC, NY = 4, 2, 4
S = NX * NC
U = 512
UB = U // S
LANES = 128
TILE = 512
TWO, THREE, FOUR, SIX = 2, 3, 4, 6
BOTH = (0, 1)
F32, BF16 = jnp.float32, jnp.bfloat16
MESH = pl.DeviceIdType.MESH
EPS = 1e-6


def nn(a, b):
    return lax.dot_general(a, b, (((1,), (0,)), ((), ())), preferred_element_type=F32)


def nt(a, b):
    return lax.dot_general(a, b, (((1,), (1,)), ((), ())), preferred_element_type=F32)


def tn(a, b):
    return lax.dot_general(a, b, (((0,), (0,)), ((), ())), preferred_element_type=F32)


def scale_of(wide):
    return lax.rsqrt(jnp.mean(wide * wide, -1, keepdims=True) + EPS)


def other(bit, by):
    return bit + by - TWO * bit * by


def glu_backward(g, u, dh):
    sig = jax.nn.sigmoid(g)
    silu = g * sig
    by_silu = dh * u
    return (silu * u).astype(BF16), (by_silu * (sig + silu * (1.0 - sig))).astype(BF16), (silu * dh).astype(BF16)


class Copy:
    def __init__(self, **what):
        self.what = what

    def __getattr__(self, name):
        return getattr(pltpu.make_async_remote_copy(**self.what), name)


def start(copies):
    for copy in copies:
        copy.start()


def arrived(copies):
    for copy in copies:
        copy.wait_recv()


def sent(copies):
    for copy in copies:
        copy.wait_send()


def done(copies):
    for copy in copies:
        copy.wait()


def prep_kernel(wg, wu, wd, wgu, wdn, block, sem, *, units):
    layers, rows, _ = wg.shape
    s = lax.axis_index("s")
    x, c = lax.div(s, NC), lax.rem(s, NC)
    low = lax.broadcasted_iota(jnp.int32, (rows, LANES), 1) < UB
    copies = []
    for l in range(layers):
        for j in range(units):
            copies.append(pltpu.make_async_copy(wd.at[l, j], wdn.at[l * units + j, x, c], sem.at[1, l, j]))
    start(copies)
    for l in range(layers):
        for j in range(units):
            for h, w in enumerate((wg, wu)):
                for a in range(NX):
                    swap = j % TWO
                    first = (TWO * a + swap) * units + j
                    second = (TWO * a + 1 - swap) * units + j
                    one = w[l, :, pl.ds(first // TWO * LANES, LANES)]
                    two = w[l, :, pl.ds(second // TWO * LANES, LANES)]
                    block[l, j, h, :, pl.ds(a * LANES, LANES)] = jnp.where(low, one, two)
            copy = pltpu.make_async_copy(block.at[l, j], wgu.at[l * units + j, :, x, c], sem.at[0, l, j])
            copy.start()
            copies.append(copy)
    done(copies)


def prep(w_gate, w_up, w_down):
    layers, rows, ff = w_gate.shape
    units, d = ff // U, w_down.shape[-1]
    anywhere = pl.BlockSpec(memory_space=pl.ANY)
    return pl.pallas_call(
        functools.partial(prep_kernel, units=units),
        in_specs=[pl.BlockSpec(memory_space=pltpu.VMEM)] * 3,
        out_specs=[anywhere] * 2,
        out_shape=[jax.ShapeDtypeStruct((layers * units, 2, NX, NC, rows, U), BF16), jax.ShapeDtypeStruct((layers * units, NX, NC, UB, d), BF16)],
        scratch_shapes=[pltpu.VMEM((layers, units, 2, rows, U), BF16), pltpu.SemaphoreType.DMA((2, layers, units))],
        name="prep",
    )(w_gate, w_up, w_down.reshape(layers, units, UB, d))


def layers_kernel(
    x0, dy, wgu_in, wdn_in,
    wgu, wdn, h1, a0T, silu0, slope0, hid0, fgu, fd,
    squares,
    a1, aT, dyv, acc, hid, dgt, dup, wv, wdv, upt,
    ggu, gd, pgu, pd,
    sa1, ra1, sb1, rb1, sa2, ra2, sb2, rb2, res1, res2,
    sa3, ra3, sb3, rb3, sa4, ra4, sb4, rb4, q1, q2,
    zs1, zs2, zr1, zr2, gz1, gz2, ss, sr,
    wsem, asem, tsem, hsem,
    psend, precv, s1s, s1r, s2s, s2r, s3s, s3r, s4s, s4r, zss, zsr, gss, gsr, gls, ys, yr, qss, qsr,
    xas, xar, xbs, xbr, yas, yar, ybs, ybr, dds, ddr,
    *, tile, nz,
):
    tokens, d = dyv.shape
    total_units = wgu.shape[0]
    units = total_units // TWO
    n_tiles = tokens // tile
    ngz = nz - 1
    half = ngz - ngz // TWO

    s, r = lax.axis_index("s"), lax.axis_index("r")
    x, c = lax.div(s, NC), lax.rem(s, NC)
    y, z = lax.div(r, nz), lax.rem(r, nz)
    turn = lambda i, by, n: lax.rem(i + by + n, n)
    x_dev = lambda k: {"s": turn(x, k, NX) * NC + c}
    y_dev = lambda k: {"r": turn(y, k, NY) * nz + z}
    z_dev = lambda k: {"r": y * nz + k}
    partner = {"s": x * NC + 1 - c}
    ways = tuple(enumerate((1, -1)))

    def remote(src, dst, send, recv, dev):
        return Copy(src_ref=src, dst_ref=dst, send_sem=send, recv_sem=recv, device_id=dev, device_id_type=MESH)

    def when(condition, do):
        pl.when(condition)(do)

    barrier = pltpu.get_barrier_semaphore()
    group = [{"s": turn(s, k, S)} for k in range(1, S)]
    peers = group + [y_dev(k) for k in range(1, NY)]
    peers += [z_dev(turn(z, k, nz)) for k in range(1, nz)]
    for dev in peers:
        pl.semaphore_signal(barrier, inc=1, device_id=dev, device_id_type=MESH)
    pl.semaphore_wait(barrier, len(peers))

    def cols(k):
        return pl.ds(pl.multiple_of(k * LANES, LANES), LANES)

    def piece(v, k, q):
        return wgu.at[v, :, k, c, :, cols(q)]

    def x_first(v):
        a2 = lax.rem(v, TWO)
        for w, by in ways:
            out = [(piece(v, x, y), 0), (wdn.at[v, x, c], 1)]
            yield by, [remote(ref, ref, xas.at[a2, w, i], xar.at[a2, w, i], x_dev(by)) for ref, i in out]

    def x_second(v):
        a2 = lax.rem(v, TWO)
        for w, by in ways:
            k = turn(x, -by, NX)
            out = [(wgu.at[v, w, k, c, :, cols(y)], 0), (wdn.at[v, k, c, pl.ds(w * (UB // TWO), UB // TWO)], 1)]
            yield by, [remote(ref, ref, xbs.at[a2, w, i], xbr.at[a2, w, i], x_dev(by)) for ref, i in out]

    def y_first(v, which):
        a2 = lax.rem(v, TWO)
        for w, by in ways:
            out = [(piece(v, turn(x, i, NX), y), i) for i in which]
            yield by, [remote(ref, ref, yas.at[a2, w, i], yar.at[a2, w, i], y_dev(by)) for ref, i in out]

    def y_second(v, which):
        a2 = lax.rem(v, TWO)
        for w, by in ways:
            out = [(wgu.at[v, w, turn(x, i, NX), c, :, cols(turn(y, -by, NY))], i) for i in which]
            yield by, [remote(ref, ref, ybs.at[a2, w, i], ybr.at[a2, w, i], y_dev(by)) for ref, i in out]

    def across(v):
        a2 = lax.rem(v, TWO)
        out = [(wgu.at[v, :, :, c], 0), (wdn.at[v, :, c], 1)]
        return [remote(ref, ref, dds.at[a2, i], ddr.at[a2, i], partner) for ref, i in out]

    def every(groups):
        return [copy for _, group in groups for copy in group]

    near, far = (1, NX - 1), (TWO,)

    def g1(v):
        start(every(x_first(v)))

    def g2(v):
        arrived(every(x_first(v)))
        start(every(x_second(v)))
        start(every(y_first(v, near)))

    def g3(v):
        arrived(every(x_second(v)))
        start(every(y_first(v, far)))
        arrived(every(y_first(v, near)))
        start(every(y_second(v, near)))
        sent(every(x_first(v)))

    def g4(v):
        arrived(every(y_first(v, far)))
        start(every(y_second(v, far)))
        arrived(every(y_second(v, near)))
        sent(every(x_second(v)))
        sent(every(y_first(v, near)))

    def g5(v):
        arrived(every(y_second(v, far)))
        start(across(v))
        sent(every(y_first(v, far)))
        sent(every(y_second(v, near)))

    def g6(v):
        arrived(across(v))
        sent(across(v))
        sent(every(y_second(v, far)))
        start(weights(v))

    stages = (g1, g2, g3, g4, g5, g6)

    def gather(*what):
        for number, v in what:
            with jax.named_scope(f"g{number}"):
                when(v < total_units, functools.partial(stages[number - 1], v))

    def gather_beside(v, i):
        ahead = (((4, 2),), ((3, 3),), ((6, 1), (2, 4)), ((5, 2), (1, 5)))[i]
        gather(*((number, v + by) for number, by in ahead))

    def weights(v, down_only=False):
        slot, unit = lax.rem(v, TWO), lax.rem(v, total_units)
        swap = lax.rem(lax.rem(unit, units), TWO)
        copies = [] if down_only else [pltpu.make_async_copy(wgu.at[unit, h], wv.at[slot, h], wsem.at[slot, h]) for h in BOTH]
        for q in BOTH:
            copies.append(pltpu.make_async_copy(wdn.at[unit, :, q], wdv.at[slot, :, other(q, swap)], wsem.at[slot, TWO + q]))
        return copies

    class Ring:
        def __init__(self, me, dev, get, put, buffers, send, recv):
            self.me, self.get, self.put = me, get, put
            self.sa, self.ra, self.sb, self.rb = buffers
            self.a = [remote(self.sa(w), self.ra(w), send.at[w], recv.at[w], dev(by)) for w, by in ways]
            at = lambda w, h: TWO + TWO * w + h
            self.b = [[remote(self.sb(w, h), self.rb(w, h), send.at[at(w, h)], recv.at[at(w, h)], dev(by)) for h in BOTH] for w, by in ways]

        def start(self):
            for h in BOTH:
                self.sa(h)[...] = self.get(turn(self.me, TWO, FOUR), h).astype(BF16)
                self.a[h].start()
            for w, by in ways:
                self.sb(w, 1 - w)[...] = self.get(turn(self.me, by, FOUR), 1 - w).astype(BF16)
                self.b[w][1 - w].start()

        def middle(self):
            for h, by in ways:
                self.a[h].wait_recv()
                self.sb(h, h)[...] = (self.get(turn(self.me, by, FOUR), h) + self.ra(h)[...].astype(F32)).astype(BF16)
                self.b[h][h].start()
            sent(self.a)

        def end(self):
            for w in BOTH:
                arrived(self.b[w])
            for h in BOTH:
                self.put(h, self.get(self.me, h) + self.rb(0, h)[...].astype(F32) + self.rb(1, h)[...].astype(F32))
            for w in BOTH:
                sent(self.b[w])

    def slots(u):
        return lax.rem(u, TWO), lax.rem(u, THREE), lax.rem(lax.rem(u, units), TWO)

    def ring1(u):
        a2, p, _ = slots(u)

        def get(k, h):
            return ggu[a2, h, k, c].astype(F32) + pgu[p, h, k].astype(F32)

        def put(h, total):
            for k in range(NY):
                res1[k, h] = total[:, k * LANES : (k + 1) * LANES]

        buffers = lambda h: sa1.at[h], lambda h: ra1.at[a2, h], lambda w, h: sb1.at[a2, w, h], lambda w, h: rb1.at[p, w, h]
        return Ring(x, x_dev, get, put, buffers, s1s.at[a2], s1r.at[p])

    def ring2(u):
        a2, p, swap = slots(u)
        pos = other(c, swap)

        def get(k, h):
            return gd[a2, pl.ds(TWO * h, TWO), pos, k].astype(F32) + pd[p, pl.ds(TWO * h, TWO), k].astype(F32)

        def put(h, total):
            res2[pl.ds(TWO * h, TWO)] = total

        buffers = lambda h: sa2.at[h], lambda h: ra2.at[a2, h], lambda w, h: sb2.at[a2, w, h], lambda w, h: rb2.at[p, w, h]
        return Ring(y, y_dev, get, put, buffers, s2s.at[a2], s2r.at[p])

    def ring3(u):
        a2, _, _ = slots(u)

        def get(k, h):
            return res1[k, h]

        def put(h, total):
            rows = total.shape[0] // ngz
            for k in range(ngz):
                q1[k, h] = total[k * rows : (k + 1) * rows]

        buffers = lambda h: sa3.at[h], lambda h: ra3.at[a2, h], lambda w, h: sb3.at[w, h], lambda w, h: rb3.at[a2, w, h]
        return Ring(y, y_dev, get, put, buffers, s3s, s3r.at[a2])

    cut = [pl.ds(0, U), pl.ds(U, d - U)]

    def ring4(u):
        a2, _, _ = slots(u)

        def get(k, h):
            return res2[k, :, cut[h]]

        def put(h, total):
            q2[:, cut[h]] = total

        buffers = lambda h: sa4.at[:, cut[h]], lambda h: ra4.at[a2, :, cut[h]], lambda w, h: sb4.at[w, :, cut[h]], lambda w, h: rb4.at[a2, w, :, cut[h]]
        return Ring(x, x_dev, get, put, buffers, s4s, s4r.at[a2])

    def to_partner(u):
        a2, p, swap = slots(u)
        ends = [(ggu.at[a2, h, :, 1 - c], pgu.at[p, h]) for h in BOTH] + [(gd.at[a2, :, other(1 - c, swap)], pd.at[p])]
        return [remote(src, dst, psend.at[i], precv.at[p, i], partner) for i, (src, dst) in enumerate(ends)]

    def c1(u):
        copies = to_partner(u)
        arrived(copies[:TWO])
        ring1(u).start()
        arrived(copies[TWO:])
        ring2(u).start()
        sent(copies)

    def c2(u):
        ring1(u).middle()
        ring2(u).middle()

    def c3(u):
        ring1(u).end()
        ring3(u).start()
        ring2(u).end()
        ring4(u).start()

    def c4(u):
        ring3(u).middle()
        ring4(u).middle()

    def others(n, do):
        def one(k, _):
            when(k != z, functools.partial(do, k))
            return 0

        lax.fori_loop(0, n, one, 0)

    def z_copies(u, k, sender=None):
        a2 = lax.rem(u, TWO)
        sender = z if sender is None else sender
        ends = (zs1.at[k], zr1.at[a2, sender]), (zs2.at[k], zr2.at[a2, sender])
        return [remote(src, dst, zss.at[k, i], zsr.at[a2, sender, i], z_dev(k)) for i, (src, dst) in enumerate(ends)]

    def c5(u):
        ring3(u).end()
        ring4(u).end()
        width = d // ngz
        for k in range(ngz):
            zs1[k] = q1[k].astype(BF16)
            zs2[k] = q2[:, pl.ds(k * width, width)].astype(BF16)
        others(ngz, lambda k: start(z_copies(u, k)))

    def gather_copies(u, k, sender=None):
        a4 = lax.rem(u, FOUR)
        sender = z if sender is None else sender
        ends = (gz1.at[a4], fgu.at[u, y, sender]), (gz2.at[a4], fd.at[u, y, sender])
        return [remote(src, dst, gss.at[a4, k, i], gsr.at[a4, sender, i], z_dev(k)) for i, (src, dst) in enumerate(ends)]

    def own_copies(u):
        a4 = lax.rem(u, FOUR)
        ends = (gz1.at[a4], fgu.at[u, y, z]), (gz2.at[a4], fd.at[u, y, z])
        return [pltpu.make_async_copy(src, dst, gls.at[a4, i]) for i, (src, dst) in enumerate(ends)]

    def c6(u):
        a2 = lax.rem(u, TWO)

        def sums():
            others(nz, lambda k: arrived(z_copies(u, 0, k)))
            zone, width = lax.rem(z, ngz), d // ngz
            one, two = q1[zone], q2[:, pl.ds(pl.multiple_of(zone * width, LANES), width)]
            for k in range(nz):
                one += jnp.where(k == z, 0.0, zr1[a2, k].astype(F32))
                two += jnp.where(k == z, 0.0, zr2[a2, k].astype(F32))
            one, two = one.astype(BF16), two.astype(BF16)
            a4 = lax.rem(u, FOUR)
            gz1[a4], gz2[a4] = one, two
            one, two = one.astype(F32), two.astype(F32)
            ss[...] += jnp.full(ss.shape, jnp.sum(one * one) + jnp.sum(two * two))
            start(own_copies(u))
            others(nz, lambda k: start(gather_copies(u, k)))

        when(z < ngz, sums)
        others(ngz, lambda k: sent(z_copies(u, k)))

    def y_copies(u, by, second, sender_y=None):
        a4 = lax.rem(u, FOUR)
        w = 0 if by > 0 else 1
        if not second:
            ends = fgu.at[u, y], fd.at[u, y]
        else:
            k = turn(y, -by, NY)
            ends = fgu.at[u, k, :, w], fd.at[u, k, (pl.ds(0, half), pl.ds(half, ngz - half))[w]]
        return [remote(ref, ref, ys.at[a4, w, second, i], yr.at[a4, w, second, i], y_dev(by)) for i, ref in enumerate(ends)]

    def c7(u):
        others(ngz, lambda k: arrived(gather_copies(u, 0, k)))

        def mine():
            done(own_copies(u))
            others(nz, lambda k: sent(gather_copies(u, k)))

        when(z < ngz, mine)
        for _, by in ways:
            start(y_copies(u, by, 0))

    def c8(u):
        for _, by in ways:
            arrived(y_copies(u, by, 0))
            start(y_copies(u, by, 1))
            sent(y_copies(u, by, 0))

    def c9(u):
        for _, by in ways:
            arrived(y_copies(u, by, 1))
            sent(y_copies(u, by, 1))

    plan = {0: ((c7, 4),), 1: ((c9, 5), (c5, 3), (c1, 1)), 2: ((c3, 2),), 3: ((c8, 4), (c6, 3)), 4: ((c4, 2), (c2, 1))}

    def steps(t, place):
        for step, behind in plan[place]:
            u = t - behind
            with jax.named_scope(step.__name__):
                when((u >= 0) & (u < total_units), functools.partial(step, u))

    def rows_of(i):
        return pl.ds(pl.multiple_of(i * tile, tile), tile)

    def weight_gradients(t):
        a2 = lax.rem(t, TWO)
        copies = to_partner(t)
        for h, by in enumerate((dgt, dup)):
            with jax.named_scope("dwgu"):
                ggu[a2, h] = nn(aT[...], by[...]).astype(BF16).reshape(ggu.shape[TWO:])
            copies[h].start()
            steps(t, THREE + h)
        with jax.named_scope("dwd"):
            gd[a2] = tn(hid[...], dyv[...]).astype(BF16).reshape(gd.shape[1:])
        copies[TWO].start()

    load = pltpu.make_async_copy(x0, dyv, asem.at[0])
    load.start()
    g1(0)
    ss[...] = jnp.zeros(ss.shape, F32)
    load.wait()
    keep = pltpu.make_async_copy(aT, a0T, asem.at[1])

    def norm(i, _):
        rows = rows_of(i)
        wide = dyv[rows].astype(F32)
        wide = wide * scale_of(wide)
        a1[rows] = wide.astype(BF16)
        aT[:, rows] = wide.T.astype(BF16)
        acc[0, rows] = jnp.zeros((tile, d), F32)
        return 0

    lax.fori_loop(0, n_tiles, norm, 0)
    keep.start()

    for number, v in (
        (2, 0), (1, 1), (3, 0), (4, 0), (2, 1), (5, 0), (3, 1), (1, 2), (6, 0), (4, 1), (2, 2), (1, 3), (5, 1), (3, 2), (2, 3), (1, 4),
    ):
        if v < total_units:
            stages[number - 1](v)

    def out_tile(j, i):
        slot = i % TWO
        at, rows = pl.ds(slot * tile, tile), pl.ds(i * tile, tile)
        return [
            pltpu.make_async_copy(acc.at[1, at, pl.ds(0, U)], silu0.at[j, rows], tsem.at[slot, 0]),
            pltpu.make_async_copy(upt.at[at], slope0.at[j, rows], tsem.at[slot, 1]),
        ]

    def out_hidden(j, i):
        rows = pl.ds(i * tile, tile)
        return [pltpu.make_async_copy(hid.at[rows], hid0.at[j, rows], hsem.at[i])]

    def forward(j, _):
        slot = lax.rem(j, TWO)
        done(weights(j))
        w_g, w_u, w_d = wv[slot, 0].reshape(d, U), wv[slot, 1].reshape(d, U), wdv[slot].reshape(U, d)
        for i in range(n_tiles):
            rows = pl.ds(i * tile, tile)
            at = pl.ds(i % TWO * tile, tile)
            if i < TWO:
                when(j > 0, lambda: done(out_tile(j, i)))
            else:
                done(out_tile(j, i))
            when(j > 0, lambda: done(out_hidden(j, i)))
            with jax.named_scope("t_fwd"):
                g, u = nn(a1[rows], w_g), nn(a1[rows], w_u)
                sig = jax.nn.sigmoid(g)
                silu = g * sig
                acc[1, at, pl.ds(0, U)], upt[at] = silu, u * (sig + silu * (1.0 - sig))
                one = (silu * u).astype(BF16)
                hid[rows] = one
                acc[0, rows] += nn(one, w_d)
            start(out_tile(j, i) + out_hidden(j, i))
            gather_beside(j, i)
        return 0

    with jax.named_scope("loop_forward"):
        lax.fori_loop(0, units, forward, 0)
    for i in range(min(TWO, n_tiles)):
        done(out_tile(0, i))
    for i in range(n_tiles):
        done(out_hidden(0, i))
    keep.wait()

    def between(i, _):
        rows = rows_of(i)
        h = dyv[rows] + acc[0, rows].astype(BF16)
        hid[rows], dgt[rows, cut_low] = h[:, :U], h[:, U:]
        pltpu.make_async_copy(dy.at[rows], dyv.at[rows], asem.at[0]).start()
        wide = h.astype(F32)
        wide = wide * scale_of(wide)
        a1[rows] = wide.astype(BF16)
        aT[:, rows] = wide.T.astype(BF16)
        for h in BOTH:
            acc[h, rows] = jnp.zeros((tile, d), F32)
        return 0

    cut_low = pl.ds(0, d - U)
    lax.fori_loop(0, n_tiles, between, 0)
    keep = [pltpu.make_async_copy(hid, h1.at[:, cut[0]], asem.at[1]), pltpu.make_async_copy(dgt.at[:, cut_low], h1.at[:, cut[1]], asem.at[TWO])]
    start(keep)
    pltpu.make_async_copy(dy, dyv, asem.at[0]).wait()
    done(keep)

    def both_passes(t, _):
        v = t + units
        slot = lax.rem(v, TWO)
        steps(t, 0)
        when(t == units - 1, lambda: start(weights(total_units, True)))
        done(weights(v))
        w_g, w_u, w_d = wv[slot, 0].reshape(d, U), wv[slot, 1].reshape(d, U), wdv[slot].reshape(U, d)
        for i in range(n_tiles):
            rows = pl.ds(i * tile, tile)
            with jax.named_scope("t_both"):
                g, u = nn(a1[rows], w_g), nn(a1[rows], w_u)
                dh = nt(dyv[rows], w_d).astype(BF16).astype(F32)
                hid[rows], by_gate, by_up = glu_backward(g, u, dh)
                dgt[rows], dup[rows] = by_gate, by_up
                acc[0, rows] += nt(by_up, w_u)
                acc[1, rows] += nt(by_gate, w_g)
            gather_beside(v, i)
            if i == 1:
                steps(t, 1)
        steps(t, TWO)
        weight_gradients(t)
        return 0

    with jax.named_scope("loop_both_passes"):
        lax.fori_loop(0, units, both_passes, 0)

    loads = [pltpu.make_async_copy(h1, a1, asem.at[0]), pltpu.make_async_copy(a0T, aT, asem.at[1])]
    start(loads)
    loads[0].wait()

    def cotangent(i, _):
        rows = rows_of(i)
        wide = a1[rows].astype(F32)
        scale = scale_of(wide)
        by_a = (acc[0, rows].astype(BF16).astype(F32) + acc[1, rows].astype(BF16).astype(F32)).astype(BF16).astype(F32)
        inner = jnp.sum(wide * by_a, -1, keepdims=True)
        by_h = by_a * scale - wide * (inner * (scale * scale * scale) * (1.0 / d))
        dyv[rows] = (dyv[rows].astype(F32) + by_h.astype(BF16).astype(F32)).astype(BF16)
        return 0

    lax.fori_loop(0, n_tiles, cotangent, 0)
    loads[1].wait()

    def in_tile(j, i):
        rows = pl.ds(i * tile, tile)
        ends = (silu0, 0), (slope0, 1)
        return [pltpu.make_async_copy(src.at[j, rows], acc.at[h, rows, pl.ds(0, U)], tsem.at[TWO + i, h]) for src, h in ends]

    for i in range(n_tiles):
        start(in_tile(0, i))

    def backward_only(t, _):
        j = t - units
        v = t + units
        slot = lax.rem(v, TWO)
        hidden = pltpu.make_async_copy(hid0.at[j], hid, hsem.at[0])
        hidden.start()
        steps(t, 0)
        when(j < units - 1, lambda: start(weights(v + 1, True)))
        done(weights(v, True))
        w_d = wdv[slot].reshape(U, d)
        for i in range(n_tiles):
            rows = pl.ds(i * tile, tile)
            done(in_tile(j, i))
            with jax.named_scope("t_back"):
                dh = nt(dyv[rows], w_d).astype(BF16).astype(F32)
                dup[rows] = (acc[0, rows, pl.ds(0, U)] * dh).astype(BF16)
                dgt[rows] = (acc[1, rows, pl.ds(0, U)] * dh).astype(BF16)
            if i == 1:
                steps(t, 1)
        steps(t, TWO)

        def ahead():
            for i in range(n_tiles):
                start(in_tile(j + 1, i))

        when(j < units - 1, ahead)
        hidden.wait()
        weight_gradients(t)
        return 0

    with jax.named_scope("loop_backward_only"):
        lax.fori_loop(units, total_units, backward_only, 0)

    last = total_units - 1
    for do, before in (
        (c5, 2), (c3, 1), (c7, 3), (c9, 4), (c1, 0), (c4, 1), (c6, 2), (c8, 3), (c2, 0), (c5, 1), (c3, 0), (c6, 1), (c4, 0), (c7, 2), (c5, 0), (c6, 0),
    ):
        if before <= last:
            do(last - before)

    def exchange(number, devs):
        copies = [remote(ss, sr.at[number, i], qss.at[number, i], qsr.at[number, i], dev) for i, dev in enumerate(devs)]
        start(copies)

        def finish():
            arrived(copies)
            sent(copies)
            total = ss[...]
            for i in range(len(devs)):
                total += sr[number, i]
            ss[...] = total

        return finish

    rings = [z_dev(turn(z, k, nz)) for k in range(1, nz)], [y_dev(k) for k in range(1, NY)], group
    rest = ((c7, 1), (c8, 2), (c9, 3), (c7, 0)), ((c8, 1), (c9, 2), (c8, 0)), ((c9, 1), (c9, 0))
    for number, devs in enumerate(rings):
        finish = exchange(number, devs)
        for do, before in rest[number]:
            do(last - before)
        finish()
    squares[...] = ss[...]


def layers(x, dy, wgu, wdn, nz):
    tokens, d = x.shape
    units = wgu.shape[0] // TWO
    tile = TILE
    n_tiles = tokens // tile
    rg, ngz = d // S, nz - 1
    rz, cz, rd = rg // ngz, d // ngz, UB // NY
    vmem = lambda *shape, dtype=BF16: pltpu.VMEM(shape, dtype)
    slots = lambda *shape: [vmem(*lead, *shape) for lead in ((TWO,), (TWO, TWO), (TWO, TWO, TWO), (THREE, TWO, TWO))]
    small = lambda *shape: [vmem(*lead, *shape) for lead in ((TWO,), (TWO, TWO), (TWO, TWO), (TWO, TWO, TWO))]
    narrow = lambda *shape: [vmem(*lead, *shape) for lead in ((), (TWO,), (TWO,), (TWO, TWO))]
    dma = lambda *shape: pltpu.SemaphoreType.DMA(shape)
    scratch = [
        vmem(tokens, d), vmem(d, tokens), vmem(tokens, d), vmem(TWO, tokens, d, dtype=F32),
        vmem(tokens, U), vmem(tokens, U), vmem(tokens, U),
        vmem(TWO, TWO, NX, NC, rg, U), vmem(TWO, NX, NC, UB, d), vmem(min(TWO, n_tiles) * tile, U, dtype=F32),
        vmem(TWO, TWO, NX, NC, rg, U), vmem(TWO, NX, NC, NY, rd, d), vmem(THREE, TWO, NX, rg, U), vmem(THREE, NX, NY, rd, d),
        *slots(rg, U), *slots(TWO, rd, d),
        vmem(NY, TWO, rg, LANES, dtype=F32), vmem(NX, rd, d, dtype=F32),
        *small(rg, LANES), *narrow(rd, d),
        vmem(ngz, TWO, rz, LANES, dtype=F32), vmem(rd, d, dtype=F32),
        vmem(ngz, TWO, rz, LANES), vmem(ngz, rd, cz), vmem(TWO, nz, TWO, rz, LANES), vmem(TWO, nz, rd, cz),
        vmem(FOUR, TWO, rz, LANES), vmem(FOUR, rd, cz), vmem(S, LANES, dtype=F32), vmem(THREE, S, S, LANES, dtype=F32),
        dma(TWO, FOUR), dma(THREE), dma(TWO + n_tiles, TWO), dma(n_tiles),
        dma(THREE), dma(THREE, THREE), dma(TWO, SIX), dma(THREE, SIX), dma(TWO, SIX), dma(THREE, SIX), dma(SIX), dma(TWO, SIX), dma(SIX), dma(TWO, SIX),
        dma(ngz, TWO), dma(TWO, nz, TWO), dma(FOUR, nz, TWO), dma(FOUR, nz, TWO), dma(FOUR, TWO), dma(FOUR, TWO, TWO, TWO), dma(FOUR, TWO, TWO, TWO), dma(THREE, S), dma(THREE, S),
        dma(TWO, TWO, TWO), dma(TWO, TWO, TWO), dma(TWO, TWO, TWO), dma(TWO, TWO, TWO), dma(TWO, TWO, NX), dma(TWO, TWO, NX), dma(TWO, TWO, NX), dma(TWO, TWO, NX), dma(TWO, TWO), dma(TWO, TWO),
    ]
    anywhere = pl.BlockSpec(memory_space=pl.ANY)
    array = jax.ShapeDtypeStruct
    return pl.pallas_call(
        functools.partial(layers_kernel, tile=tile, nz=nz),
        in_specs=[anywhere] * FOUR,
        out_specs=[anywhere] * 9 + [pl.BlockSpec(memory_space=pltpu.VMEM)],
        out_shape=[
            array(wgu.shape, BF16),
            array(wdn.shape, BF16),
            array((tokens, d), BF16),
            array((d, tokens), BF16),
            array((units, tokens, U), F32),
            array((units, tokens, U), F32),
            array((units, tokens, U), BF16),
            array((TWO * units, NY, ngz, TWO, rz, LANES), BF16),
            array((TWO * units, NY, ngz, rd, cz), BF16),
            array((S, LANES), F32),
        ],
        scratch_shapes=scratch,
        input_output_aliases={TWO: 0, THREE: 1},
        compiler_params=pltpu.CompilerParams(collective_id=1, has_side_effects=True, vmem_limit_bytes=67043328),
        cost_estimate=pl.CostEstimate(flops=15 * TWO * tokens * d * U * units, bytes_accessed=2**28, transcendentals=0),
        name="layers",
    )(x, dy, wgu, wdn)[SIX + 1 :]


def step_kernel(squares, fgu, fd, wg, mg, vg, wu, mu, vu, wd, md, vd, *out, n_units, count):
    ngz, rd, cz = fd.shape[2:]
    fac = jnp.minimum(1.0, 0.5 * lax.rsqrt(squares[0:1] / count + 1e-30))[:, 0:1]

    def adamw(g, w, m, v):
        g = g.astype(F32) * fac
        m = 0.9 * m + 0.1 * g
        v = 0.95 * v + 0.05 * g * g
        step = m * lax.rsqrt(v + 1e-8) + 0.1 * w.astype(F32)
        return (w.astype(F32) - 0.02 * step).astype(BF16), m, v

    rows = wg.shape[1]
    low = lax.broadcasted_iota(jnp.int32, (rows, LANES), 1) < UB
    for h, (w, m, v, outs) in enumerate(((wg, mg, vg, out[0::THREE]), (wu, mu, vu, out[1::THREE]))):
        by_unit = [jnp.concatenate([fgu[j, 0, k, h] for k in range(ngz)], axis=0).astype(F32) for j in range(n_units)]
        for i in range(n_units):
            at = pl.ds(i * LANES, LANES)
            g = jnp.where(low, by_unit[TWO * i % n_units], by_unit[(TWO * i + 1) % n_units])
            outs[0][0, :, at], outs[1][0, :, at], outs[2][0, :, at] = adamw(g, w[0, :, at], m[0, :, at], v[0, :, at])
    outs = out[TWO::THREE]
    for j in range(n_units):
        g = jnp.concatenate([fd[j, 0, k] for k in range(ngz)], axis=1)
        outs[0][0, j, 0], outs[1][0, j, 0], outs[2][0, j, 0] = adamw(g, wd[0, j, 0], md[0, j, 0], vd[0, j, 0])


def optimizer(squares, fgu, fd, weights, m, v):
    layers, rg, ff = weights[0].shape
    n_units = ff // U
    d = weights[2].shape[2]
    _, _, ngz, rd, cz = fd.shape
    rz = rg // ngz
    wide = ff // NY
    down = lambda a: a.reshape(layers, n_units, NY, rd, d)
    col = pl.BlockSpec((1, rg, wide), lambda l, a: (l, 0, a))
    row = pl.BlockSpec((1, n_units, 1, rd, d), lambda l, a: (l, 0, a, 0, 0))
    args = []
    for i in range(3):
        args += [w if i < 2 else down(w) for w in (weights[i], m[i], v[i])]
    shapes = lambda dtype: [jax.ShapeDtypeStruct((layers, rg, ff), dtype)] * 2 + [jax.ShapeDtypeStruct((layers, n_units, NY, rd, d), dtype)]
    out = pl.pallas_call(
        functools.partial(step_kernel, n_units=n_units, count=S * sum(w.size for w in weights)),
        grid=(layers, NY),
        in_specs=[
            pl.BlockSpec((S, LANES), lambda l, a: (0, 0)),
            pl.BlockSpec((n_units, 1, ngz, 2, rz, LANES), lambda l, a: (1 - l, a, 0, 0, 0, 0)),
            pl.BlockSpec((n_units, 1, ngz, rd, cz), lambda l, a: (1 - l, a, 0, 0, 0)),
        ]
        + [col] * 6
        + [row] * 3,
        out_specs=[col, col, row] * 3,
        out_shape=shapes(BF16) + shapes(F32) + shapes(F32),
        name="adamw",
    )(squares, fgu, fd, *args)
    return tuple(o.reshape(layers, -1, d) if i % 3 == 2 else o for i, o in enumerate(out))


def solution(mesh):
    nz = mesh.shape["r"] // NY

    def step(x, dy, *arrays):
        weights, m, v = (arrays[i : i + THREE] for i in (0, THREE, SIX))
        fgu, fd, squares = layers(x[0], dy[0], *prep(*weights), nz)
        return optimizer(squares, fgu, fd, weights, m, v)

    states, cut = P(("rep", "r", "s"), None, None), P(None, "s", None)
    return jax.shard_map(
        step,
        mesh=mesh,
        in_specs=(states, states) + (cut,) * 9,
        out_specs=(P("rep", "s", None),) * 9,
        check_vma=False,
    )
```

```python
import functools

import jax
import jax.numpy as jnp
from jax import lax
from jax.experimental import pallas as pl
from jax.experimental.pallas import tpu as pltpu
from jax.sharding import PartitionSpec as P

NX, NC, NY = 4, 2, 4
S = NX * NC
U = 512
UB = U // S
LANES = 128
TILE = 512
TWO, THREE, FOUR, SIX = 2, 3, 4, 6
BOTH = (0, 1)
F32, BF16 = jnp.float32, jnp.bfloat16
MESH = pl.DeviceIdType.MESH
EPS = 1e-6


def nn(a, b):
    return lax.dot_general(a, b, (((1,), (0,)), ((), ())), preferred_element_type=F32)


def nt(a, b):
    return lax.dot_general(a, b, (((1,), (1,)), ((), ())), preferred_element_type=F32)


def tn(a, b):
    return lax.dot_general(a, b, (((0,), (0,)), ((), ())), preferred_element_type=F32)


def scale_of(wide):
    return lax.rsqrt(jnp.mean(wide * wide, -1, keepdims=True) + EPS)


def other(bit, by):
    return bit + by - TWO * bit * by


def glu_backward(g, u, dh):
    sig = jax.nn.sigmoid(g)
    silu = g * sig
    by_silu = dh * u
    return (silu * u).astype(BF16), (by_silu * (sig + silu * (1.0 - sig))).astype(BF16), (silu * dh).astype(BF16)


class Copy:
    def __init__(self, **what):
        self.what = what

    def __getattr__(self, name):
        return getattr(pltpu.make_async_remote_copy(**self.what), name)


def start(copies):
    for copy in copies:
        copy.start()


def arrived(copies):
    for copy in copies:
        copy.wait_recv()


def sent(copies):
    for copy in copies:
        copy.wait_send()


def done(copies):
    for copy in copies:
        copy.wait()


def prep_kernel(wg, wu, wd, wgu, wdn, block, sem, *, units):
    layers, rows, _ = wg.shape
    s = lax.axis_index("s")
    x, c = lax.div(s, NC), lax.rem(s, NC)
    low = lax.broadcasted_iota(jnp.int32, (rows, LANES), 1) < UB
    copies = []
    for l in range(layers):
        for j in range(units):
            copies.append(pltpu.make_async_copy(wd.at[l, j], wdn.at[l * units + j, x, c], sem.at[1, l, j]))
    start(copies)
    for l in range(layers):
        for j in range(units):
            for h, w in enumerate((wg, wu)):
                for a in range(NX):
                    swap = j % TWO
                    first = (TWO * a + swap) * units + j
                    second = (TWO * a + 1 - swap) * units + j
                    one = w[l, :, pl.ds(first // TWO * LANES, LANES)]
                    two = w[l, :, pl.ds(second // TWO * LANES, LANES)]
                    block[l, j, h, :, pl.ds(a * LANES, LANES)] = jnp.where(low, one, two)
            copy = pltpu.make_async_copy(block.at[l, j], wgu.at[l * units + j, :, x, c], sem.at[0, l, j])
            copy.start()
            copies.append(copy)
    done(copies)


def prep(w_gate, w_up, w_down):
    layers, rows, ff = w_gate.shape
    units, d = ff // U, w_down.shape[-1]
    anywhere = pl.BlockSpec(memory_space=pl.ANY)
    return pl.pallas_call(
        functools.partial(prep_kernel, units=units),
        in_specs=[pl.BlockSpec(memory_space=pltpu.VMEM)] * 3,
        out_specs=[anywhere] * 2,
        out_shape=[jax.ShapeDtypeStruct((layers * units, 2, NX, NC, rows, U), BF16), jax.ShapeDtypeStruct((layers * units, NX, NC, UB, d), BF16)],
        scratch_shapes=[pltpu.VMEM((layers, units, 2, rows, U), BF16), pltpu.SemaphoreType.DMA((2, layers, units))],
        name="prep",
    )(w_gate, w_up, w_down.reshape(layers, units, UB, d))


def layers_kernel(
    x0, dy, wgu_in, wdn_in,
    wgu, wdn, h1, a0T, silu0, slope0, hid0, fgu, fd,
    squares,
    a1, aT, dyv, acc, hid, dgt, dup, wv, wdv, upt,
    ggu, gd, pgu, pd,
    sa1, ra1, sb1, rb1, sa2, ra2, sb2, rb2, res1, res2,
    sa3, ra3, sb3, rb3, sa4, ra4, sb4, rb4, q1, q2,
    zs1, zs2, zr1, zr2, gz1, gz2, ss, sr,
    wsem, asem, tsem, hsem,
    psend, precv, s1s, s1r, s2s, s2r, s3s, s3r, s4s, s4r, zss, zsr, gss, gsr, gls, ys, yr, qss, qsr,
    xas, xar, xbs, xbr, yas, yar, ybs, ybr, dds, ddr,
    *, tile, nz,
):
    tokens, d = dyv.shape
    total_units = wgu.shape[0]
    units = total_units // TWO
    n_tiles = tokens // tile
    ngz = nz - 1

    s, r = lax.axis_index("s"), lax.axis_index("r")
    x, c = lax.div(s, NC), lax.rem(s, NC)
    y, z = lax.div(r, nz), lax.rem(r, nz)
    turn = lambda i, by, n: lax.rem(i + by + n, n)
    x_dev = lambda k: {"s": turn(x, k, NX) * NC + c}
    y_dev = lambda k: {"r": turn(y, k, NY) * nz + z}
    z_dev = lambda k: {"r": y * nz + k}
    partner = {"s": x * NC + 1 - c}
    ways = tuple(enumerate((1, -1)))

    def remote(src, dst, send, recv, dev):
        return Copy(src_ref=src, dst_ref=dst, send_sem=send, recv_sem=recv, device_id=dev, device_id_type=MESH)

    def when(condition, do):
        pl.when(condition)(do)

    barrier = pltpu.get_barrier_semaphore()
    group = [{"s": turn(s, k, S)} for k in range(1, S)]
    peers = group + [y_dev(k) for k in range(1, NY)]
    peers += [z_dev(turn(z, k, nz)) for k in range(1, nz)]
    for dev in peers:
        pl.semaphore_signal(barrier, inc=1, device_id=dev, device_id_type=MESH)
    pl.semaphore_wait(barrier, len(peers))

    def cols(k):
        return pl.ds(pl.multiple_of(k * LANES, LANES), LANES)

    def piece(v, k, q):
        return wgu.at[v, :, k, c, :, cols(q)]

    GU, DOWN = (0,), (1,)

    def x_first(v, which):
        a2 = lax.rem(v, TWO)
        for w, by in ways:
            out = [((piece(v, x, y), wdn.at[v, x, c])[i], i) for i in which]
            yield by, [remote(ref, ref, xas.at[a2, w, i], xar.at[a2, w, i], x_dev(by)) for ref, i in out]

    def x_second(v, which):
        a2 = lax.rem(v, TWO)
        for w, by in ways:
            k = turn(x, -by, NX)
            out = [((wgu.at[v, w, k, c, :, cols(y)], wdn.at[v, k, c, pl.ds(w * (UB // TWO), UB // TWO)])[i], i) for i in which]
            yield by, [remote(ref, ref, xbs.at[a2, w, i], xbr.at[a2, w, i], x_dev(by)) for ref, i in out]

    def y_first(v, which):
        a2 = lax.rem(v, TWO)
        for w, by in ways:
            out = [(piece(v, turn(x, i, NX), y), i) for i in which]
            yield by, [remote(ref, ref, yas.at[a2, w, i], yar.at[a2, w, i], y_dev(by)) for ref, i in out]

    def y_second(v, which):
        a2 = lax.rem(v, TWO)
        for w, by in ways:
            out = [(wgu.at[v, w, turn(x, i, NX), c, :, cols(turn(y, -by, NY))], i) for i in which]
            yield by, [remote(ref, ref, ybs.at[a2, w, i], ybr.at[a2, w, i], y_dev(by)) for ref, i in out]

    def across(v, which):
        a3 = lax.rem(v, THREE)
        out = [(wgu.at[v, :, turn(x, i, NX), c] if i < NX else wdn.at[v, :, c], i) for i in which]
        return [remote(ref, ref, dds.at[a3, i], ddr.at[a3, i], partner) for ref, i in out]

    def every(groups):
        return [copy for _, group in groups for copy in group]

    near, far = (1, NX - 1), (TWO,)
    early = (0, *near, NX)

    def g1(v):
        start(every(x_first(v, GU)))

    def g2(v):
        arrived(every(x_first(v, GU)))
        start(every(x_second(v, GU)))
        start(every(y_first(v, near)))
        start(every(x_first(v, DOWN)))

    def g3(v):
        arrived(every(x_second(v, GU)))
        start(every(y_first(v, far)))
        arrived(every(y_first(v, near)))
        start(every(y_second(v, near)))
        arrived(every(x_first(v, DOWN)))
        start(every(x_second(v, DOWN)))
        sent(every(x_first(v, GU)))

    def g4(v):
        arrived(every(y_first(v, far)))
        start(every(y_second(v, far)))
        arrived(every(y_second(v, near)))
        arrived(every(x_second(v, DOWN)))
        start(across(v, early))
        sent(every(x_first(v, DOWN)))
        sent(every(x_second(v, GU)))
        sent(every(y_first(v, near)))

    def g5(v):
        arrived(every(y_second(v, far)))
        start(across(v, far))
        sent(every(x_second(v, DOWN)))
        sent(every(y_first(v, far)))
        sent(every(y_second(v, near)))

    def g6(v):
        arrived(across(v, early + far))
        sent(across(v, early + far))
        sent(every(y_second(v, far)))
        start(weights(v))

    stages = (g1, g2, g3, g4, g5, g6)

    def gather(*what):
        for number, v in what:
            with jax.named_scope(f"g{number}"):
                when(v < total_units, functools.partial(stages[number - 1], v))

    def gather_beside(v, i):
        ahead = (((4, 2),), ((3, 3),), ((6, 1), (2, 4)), ((5, 2), (1, 5)))[i]
        gather(*((number, v + by) for number, by in ahead))

    def weights(v, down_only=False):
        slot, unit = lax.rem(v, TWO), lax.rem(v, total_units)
        swap = lax.rem(lax.rem(unit, units), TWO)
        copies = [] if down_only else [pltpu.make_async_copy(wgu.at[unit, h], wv.at[slot, h], wsem.at[slot, h]) for h in BOTH]
        for q in BOTH:
            copies.append(pltpu.make_async_copy(wdn.at[unit, :, q], wdv.at[slot, :, other(q, swap)], wsem.at[slot, TWO + q]))
        return copies

    class Ring:
        def __init__(self, me, dev, get, put, buffers, send, recv):
            self.me, self.get, self.put = me, get, put
            self.sa, self.ra, self.sb, self.rb = buffers
            self.a = [remote(self.sa(w), self.ra(w), send.at[w], recv.at[w], dev(by)) for w, by in ways]
            at = lambda w, h: TWO + TWO * w + h
            self.b = [[remote(self.sb(w, h), self.rb(w, h), send.at[at(w, h)], recv.at[at(w, h)], dev(by)) for h in BOTH] for w, by in ways]

        def start(self):
            for h in BOTH:
                self.sa(h)[...] = self.get(turn(self.me, TWO, FOUR), h).astype(BF16)
                self.a[h].start()
            for w, by in ways:
                self.sb(w, 1 - w)[...] = self.get(turn(self.me, by, FOUR), 1 - w).astype(BF16)
                self.b[w][1 - w].start()

        def middle(self):
            for h, by in ways:
                self.a[h].wait_recv()
                self.sb(h, h)[...] = (self.get(turn(self.me, by, FOUR), h) + self.ra(h)[...].astype(F32)).astype(BF16)
                self.b[h][h].start()
            sent(self.a)

        def end(self):
            for w in BOTH:
                arrived(self.b[w])
            for h in BOTH:
                self.put(h, self.get(self.me, h) + self.rb(0, h)[...].astype(F32) + self.rb(1, h)[...].astype(F32))
            for w in BOTH:
                sent(self.b[w])

    def slots(u):
        return lax.rem(u, TWO), lax.rem(u, THREE), lax.rem(lax.rem(u, units), TWO)

    def ring1(u):
        a2, p, _ = slots(u)

        def get(k, h):
            return ggu[a2, h, k, c].astype(F32) + pgu[p, h, k].astype(F32)

        def put(h, total):
            for k in range(NY):
                res1[k, h] = total[:, k * LANES : (k + 1) * LANES]

        buffers = lambda h: sa1.at[h], lambda h: ra1.at[a2, h], lambda w, h: sb1.at[a2, w, h], lambda w, h: rb1.at[p, w, h]
        return Ring(x, x_dev, get, put, buffers, s1s.at[a2], s1r.at[p])

    def ring2(u):
        a2, p, swap = slots(u)
        pos = other(c, swap)

        def get(k, h):
            return gd[a2, pl.ds(TWO * h, TWO), pos, k].astype(F32) + pd[p, pl.ds(TWO * h, TWO), k].astype(F32)

        def put(h, total):
            res2[pl.ds(TWO * h, TWO)] = total

        buffers = lambda h: sa2.at[h], lambda h: ra2.at[a2, h], lambda w, h: sb2.at[a2, w, h], lambda w, h: rb2.at[p, w, h]
        return Ring(y, y_dev, get, put, buffers, s2s.at[a2], s2r.at[p])

    def ring3(u):
        a2, _, _ = slots(u)

        def get(k, h):
            return res1[k, h]

        def put(h, total):
            rows = total.shape[0] // ngz
            for k in range(ngz):
                q1[k, h] = total[k * rows : (k + 1) * rows]

        buffers = lambda h: sa3.at[h], lambda h: ra3.at[a2, h], lambda w, h: sb3.at[w, h], lambda w, h: rb3.at[a2, w, h]
        return Ring(y, y_dev, get, put, buffers, s3s, s3r.at[a2])

    cut = [pl.ds(0, U), pl.ds(U, d - U)]

    def ring4(u):
        a2, _, _ = slots(u)

        def get(k, h):
            return res2[k, :, cut[h]]

        def put(h, total):
            q2[:, cut[h]] = total

        buffers = lambda h: sa4.at[:, cut[h]], lambda h: ra4.at[a2, :, cut[h]], lambda w, h: sb4.at[w, :, cut[h]], lambda w, h: rb4.at[a2, w, :, cut[h]]
        return Ring(x, x_dev, get, put, buffers, s4s, s4r.at[a2])

    def to_partner(u):
        a2, p, swap = slots(u)
        ends = [(ggu.at[a2, h, :, 1 - c], pgu.at[p, h]) for h in BOTH] + [(gd.at[a2, :, other(1 - c, swap)], pd.at[p])]
        return [remote(src, dst, psend.at[i], precv.at[p, i], partner) for i, (src, dst) in enumerate(ends)]

    def c1(u):
        copies = to_partner(u)
        arrived(copies[:TWO])
        ring1(u).start()
        arrived(copies[TWO:])
        ring2(u).start()
        sent(copies)

    def c2(u):
        ring1(u).middle()
        ring2(u).middle()

    def c3(u):
        ring1(u).end()
        ring3(u).start()
        ring2(u).end()
        ring4(u).start()

    def c4(u):
        ring3(u).middle()
        ring4(u).middle()

    def others(n, do):
        def one(k, _):
            when(k != z, functools.partial(do, k))
            return 0

        lax.fori_loop(0, n, one, 0)

    def z_copies(u, k, sender=None):
        a2 = lax.rem(u, TWO)
        sender = z if sender is None else sender
        ends = (zs1.at[k], zr1.at[a2, sender]), (zs2.at[k], zr2.at[a2, sender])
        return [remote(src, dst, zss.at[k, i], zsr.at[a2, sender, i], z_dev(k)) for i, (src, dst) in enumerate(ends)]

    def c5(u):
        ring3(u).end()
        ring4(u).end()
        width = d // ngz
        for k in range(ngz):
            zs1[k] = q1[k].astype(BF16)
            zs2[k] = q2[:, pl.ds(k * width, width)].astype(BF16)
        others(ngz, lambda k: start(z_copies(u, k)))

    def gather_copies(u, k, sender=None):
        a4 = lax.rem(u, FOUR)
        sender = z if sender is None else sender
        ends = (gz1.at[a4], fgu.at[u, y, sender]), (gz2.at[a4], fd.at[u, y, sender])
        return [remote(src, dst, gss.at[a4, k, i], gsr.at[a4, sender, i], z_dev(k)) for i, (src, dst) in enumerate(ends)]

    def own_copies(u):
        a4 = lax.rem(u, FOUR)
        ends = (gz1.at[a4], fgu.at[u, y, z]), (gz2.at[a4], fd.at[u, y, z])
        return [pltpu.make_async_copy(src, dst, gls.at[a4, i]) for i, (src, dst) in enumerate(ends)]

    def c6(u):
        a2 = lax.rem(u, TWO)

        def sums():
            others(nz, lambda k: arrived(z_copies(u, 0, k)))
            zone, width = lax.rem(z, ngz), d // ngz
            one, two = q1[zone], q2[:, pl.ds(pl.multiple_of(zone * width, LANES), width)]
            for k in range(nz):
                one += jnp.where(k == z, 0.0, zr1[a2, k].astype(F32))
                two += jnp.where(k == z, 0.0, zr2[a2, k].astype(F32))
            one, two = one.astype(BF16), two.astype(BF16)
            a4 = lax.rem(u, FOUR)
            gz1[a4], gz2[a4] = one, two
            one, two = one.astype(F32), two.astype(F32)
            ss[...] += jnp.full(ss.shape, jnp.sum(one * one) + jnp.sum(two * two))
            start(own_copies(u))
            others(nz, lambda k: start(gather_copies(u, k)))

        when(z < ngz, sums)
        others(ngz, lambda k: sent(z_copies(u, k)))

    def y_copies(u):
        a4 = lax.rem(u, FOUR)
        ends = fgu.at[u, y], fd.at[u, y]
        return [remote(ref, ref, ys.at[a4, by, i], yr.at[a4, by, i], y_dev(by)) for by in range(1, NY) for i, ref in enumerate(ends)]

    def c7(u):
        others(ngz, lambda k: arrived(gather_copies(u, 0, k)))

        def mine():
            done(own_copies(u))
            others(nz, lambda k: sent(gather_copies(u, k)))

        when(z < ngz, mine)
        start(y_copies(u))

    def c8(u):
        arrived(y_copies(u))
        sent(y_copies(u))

    plan = {1: ((c8, 5), (c5, 3), (c1, 1)), 2: ((c3, 2), (c7, 4)), 4: ((c4, 2), (c6, 3), (c2, 1))}

    def steps(t, place):
        for step, behind in plan.get(place, ()):
            u = t - behind
            with jax.named_scope(step.__name__):
                when((u >= 0) & (u < total_units), functools.partial(step, u))

    def rows_of(i):
        return pl.ds(i * tile if isinstance(i, int) else pl.multiple_of(i * tile, tile), tile)

    def weight_gradients(t):
        a2 = lax.rem(t, TWO)
        copies = to_partner(t)
        for h, by in enumerate((dgt, dup)):
            with jax.named_scope("dwgu"):
                ggu[a2, h] = nn(aT[...], by[...]).astype(BF16).reshape(ggu.shape[TWO:])
            copies[h].start()
            steps(t, THREE + h)
        with jax.named_scope("dwd"):
            gd[a2] = tn(hid[...], dyv[...]).astype(BF16).reshape(gd.shape[1:])
        copies[TWO].start()

    load = pltpu.make_async_copy(x0, dyv, asem.at[0])
    load.start()
    g1(0)
    ss[...] = jnp.zeros(ss.shape, F32)
    load.wait()
    keep = pltpu.make_async_copy(aT, a0T, asem.at[1])

    def norm(i, _):
        rows = rows_of(i)
        wide = dyv[rows].astype(F32)
        wide = wide * scale_of(wide)
        a1[rows] = wide.astype(BF16)
        aT[:, rows] = wide.T.astype(BF16)
        acc[0, rows] = jnp.zeros((tile, d), F32)
        return 0

    lax.fori_loop(0, n_tiles, norm, 0)
    keep.start()

    for number, v in (
        (2, 0), (1, 1), (3, 0), (4, 0), (2, 1), (5, 0), (3, 1), (1, 2), (6, 0), (4, 1), (2, 2), (1, 3), (5, 1), (3, 2), (2, 3), (1, 4),
    ):
        if v < total_units:
            stages[number - 1](v)

    def out_tile(j, i):
        slot = i % TWO
        at, rows = pl.ds(slot * tile, tile), pl.ds(i * tile, tile)
        return [
            pltpu.make_async_copy(acc.at[1, at, pl.ds(0, U)], silu0.at[j, rows], tsem.at[slot, 0]),
            pltpu.make_async_copy(upt.at[at], slope0.at[j, rows], tsem.at[slot, 1]),
        ]

    def out_hidden(j, i):
        rows = pl.ds(i * tile, tile)
        return [pltpu.make_async_copy(hid.at[rows], hid0.at[j, rows], hsem.at[i])]

    def forward(j, _):
        slot = lax.rem(j, TWO)
        done(weights(j))
        w_g, w_u, w_d = wv[slot, 0].reshape(d, U), wv[slot, 1].reshape(d, U), wdv[slot].reshape(U, d)
        for i in range(n_tiles):
            rows = pl.ds(i * tile, tile)
            at = pl.ds(i % TWO * tile, tile)
            if i < TWO:
                when(j > 0, lambda: done(out_tile(j, i)))
            else:
                done(out_tile(j, i))
            when(j > 0, lambda: done(out_hidden(j, i)))
            with jax.named_scope("t_fwd"):
                g, u = nn(a1[rows], w_g), nn(a1[rows], w_u)
                sig = jax.nn.sigmoid(g)
                silu = g * sig
                acc[1, at, pl.ds(0, U)], upt[at] = silu, u * (sig + silu * (1.0 - sig))
                one = (silu * u).astype(BF16)
                hid[rows] = one
                acc[0, rows] += nn(one, w_d)
            start(out_tile(j, i) + out_hidden(j, i))
            gather_beside(j, i)
        return 0

    with jax.named_scope("loop_forward"):
        lax.fori_loop(0, units, forward, 0)
    for i in range(min(TWO, n_tiles)):
        done(out_tile(0, i))
    for i in range(n_tiles):
        done(out_hidden(0, i))
    keep.wait()

    def between(i, _):
        rows = rows_of(i)
        h = dyv[rows] + acc[0, rows].astype(BF16)
        hid[rows], dgt[rows, cut_low] = h[:, :U], h[:, U:]
        pltpu.make_async_copy(dy.at[rows], dyv.at[rows], asem.at[0]).start()
        wide = h.astype(F32)
        wide = wide * scale_of(wide)
        a1[rows] = wide.astype(BF16)
        aT[:, rows] = wide.T.astype(BF16)
        for h in BOTH:
            acc[h, rows] = jnp.zeros((tile, d), F32)
        return 0

    cut_low = pl.ds(0, d - U)
    lax.fori_loop(0, n_tiles, between, 0)
    keep = [pltpu.make_async_copy(hid, h1.at[:, cut[0]], asem.at[1]), pltpu.make_async_copy(dgt.at[:, cut_low], h1.at[:, cut[1]], asem.at[TWO])]
    start(keep)
    pltpu.make_async_copy(dy, dyv, asem.at[0]).wait()
    done(keep)

    def both_passes(t, _):
        v = t + units
        slot = lax.rem(v, TWO)
        steps(t, 0)
        when(t == units - 1, lambda: start(weights(total_units, True)))
        done(weights(v))
        w_g, w_u, w_d = wv[slot, 0].reshape(d, U), wv[slot, 1].reshape(d, U), wdv[slot].reshape(U, d)
        for i in range(n_tiles):
            rows = pl.ds(i * tile, tile)
            with jax.named_scope("t_both"):
                g, u = nn(a1[rows], w_g), nn(a1[rows], w_u)
                dh = nt(dyv[rows], w_d).astype(BF16).astype(F32)
                hid[rows], by_gate, by_up = glu_backward(g, u, dh)
                dgt[rows], dup[rows] = by_gate, by_up
                acc[0, rows] += nt(by_up, w_u)
                acc[1, rows] += nt(by_gate, w_g)
            gather_beside(v, i)
            if i == 1:
                steps(t, 1)
        when(t == units - 1, loads[0].start)
        steps(t, TWO)
        weight_gradients(t)
        return 0

    loads = [pltpu.make_async_copy(h1, a1, asem.at[0]), pltpu.make_async_copy(a0T, aT, asem.at[1])]
    with jax.named_scope("loop_both_passes"):
        lax.fori_loop(0, units, both_passes, 0)

    def in_tile(j, i):
        rows = rows_of(i)
        ends = (silu0, 0), (slope0, 1)
        return [pltpu.make_async_copy(src.at[j, rows], acc.at[h, rows, pl.ds(0, U)], tsem.at[TWO + i, h]) for src, h in ends]

    loads[1].start()
    loads[0].wait()

    def cotangent(i, _):
        rows = rows_of(i)
        wide = a1[rows].astype(F32)
        scale = scale_of(wide)
        by_a = (acc[0, rows].astype(BF16).astype(F32) + acc[1, rows].astype(BF16).astype(F32)).astype(BF16).astype(F32)
        inner = jnp.sum(wide * by_a, -1, keepdims=True)
        by_h = by_a * scale - wide * (inner * (scale * scale * scale) * (1.0 / d))
        dyv[rows] = (dyv[rows].astype(F32) + by_h.astype(BF16).astype(F32)).astype(BF16)
        start(in_tile(0, i))
        return 0

    lax.fori_loop(0, n_tiles, cotangent, 0)

    def backward_only(t, _):
        j = t - units
        v = t + units
        slot = lax.rem(v, TWO)
        hidden = pltpu.make_async_copy(hid0.at[j], hid, hsem.at[0])
        hidden.start()
        steps(t, 0)
        when(j < units - 1, lambda: start(weights(v + 1, True)))
        done(weights(v, True))
        w_d = wdv[slot].reshape(U, d)
        for i in range(n_tiles):
            rows = pl.ds(i * tile, tile)
            done(in_tile(j, i))
            with jax.named_scope("t_back"):
                dh = nt(dyv[rows], w_d).astype(BF16).astype(F32)
                dup[rows] = (acc[0, rows, pl.ds(0, U)] * dh).astype(BF16)
                dgt[rows] = (acc[1, rows, pl.ds(0, U)] * dh).astype(BF16)
            if i == 1:
                steps(t, 1)
        steps(t, TWO)

        def ahead():
            for i in range(n_tiles):
                start(in_tile(j + 1, i))

        when(j < units - 1, ahead)
        hidden.wait()
        when(j == 0, loads[1].wait)
        weight_gradients(t)
        return 0

    with jax.named_scope("loop_backward_only"):
        lax.fori_loop(units, total_units, backward_only, 0)

    last = total_units - 1
    for do, before in (
        (c5, 2), (c3, 1), (c7, 3), (c8, 4), (c1, 0), (c4, 1), (c6, 2), (c2, 0), (c5, 1), (c7, 2), (c3, 0), (c6, 1), (c4, 0), (c8, 3), (c5, 0), (c6, 0),
    ):
        if before <= last:
            with jax.named_scope("end_" + do.__name__):
                do(last - before)

    def exchange(number, devs):
        copies = [remote(ss, sr.at[number, i], qss.at[number, i], qsr.at[number, i], dev) for i, dev in enumerate(devs)]
        start(copies)

        def finish():
            arrived(copies)
            sent(copies)
            total = ss[...]
            for i in range(len(devs)):
                total += sr[number, i]
            ss[...] = total

        return finish

    rings = [z_dev(turn(z, k, nz)) for k in range(1, nz)], [y_dev(k) for k in range(1, NY)], group
    rest = ((c7, 1), (c7, 0), (c8, 2)), ((c8, 1), (c8, 0)), ()
    for number, devs in enumerate(rings):
        finish = exchange(number, devs)
        for do, before in rest[number]:
            if before <= last:
                with jax.named_scope("last_" + do.__name__):
                    do(last - before)
        with jax.named_scope("exchange"):
            finish()
    squares[...] = ss[...]


def layers(x, dy, wgu, wdn, nz):
    tokens, d = x.shape
    units = wgu.shape[0] // TWO
    tile = TILE
    n_tiles = tokens // tile
    rg, ngz = d // S, nz - 1
    rz, cz, rd = rg // ngz, d // ngz, UB // NY
    vmem = lambda *shape, dtype=BF16: pltpu.VMEM(shape, dtype)
    slots = lambda *shape: [vmem(*lead, *shape) for lead in ((TWO,), (TWO, TWO), (TWO, TWO, TWO), (THREE, TWO, TWO))]
    small = lambda *shape: [vmem(*lead, *shape) for lead in ((TWO,), (TWO, TWO), (TWO, TWO), (TWO, TWO, TWO))]
    narrow = lambda *shape: [vmem(*lead, *shape) for lead in ((), (TWO,), (TWO,), (TWO, TWO))]
    dma = lambda *shape: pltpu.SemaphoreType.DMA(shape)
    scratch = [
        vmem(tokens, d), vmem(d, tokens), vmem(tokens, d), vmem(TWO, tokens, d, dtype=F32),
        vmem(tokens, U), vmem(tokens, U), vmem(tokens, U),
        vmem(TWO, TWO, NX, NC, rg, U), vmem(TWO, NX, NC, UB, d), vmem(min(TWO, n_tiles) * tile, U, dtype=F32),
        vmem(TWO, TWO, NX, NC, rg, U), vmem(TWO, NX, NC, NY, rd, d), vmem(THREE, TWO, NX, rg, U), vmem(THREE, NX, NY, rd, d),
        *slots(rg, U), *slots(TWO, rd, d),
        vmem(NY, TWO, rg, LANES, dtype=F32), vmem(NX, rd, d, dtype=F32),
        *small(rg, LANES), *narrow(rd, d),
        vmem(ngz, TWO, rz, LANES, dtype=F32), vmem(rd, d, dtype=F32),
        vmem(ngz, TWO, rz, LANES), vmem(ngz, rd, cz), vmem(TWO, nz, TWO, rz, LANES), vmem(TWO, nz, rd, cz),
        vmem(FOUR, TWO, rz, LANES), vmem(FOUR, rd, cz), vmem(S, LANES, dtype=F32), vmem(THREE, S, S, LANES, dtype=F32),
        dma(TWO, FOUR), dma(THREE), dma(TWO + n_tiles, TWO), dma(n_tiles),
        dma(THREE), dma(THREE, THREE), dma(TWO, SIX), dma(THREE, SIX), dma(TWO, SIX), dma(THREE, SIX), dma(SIX), dma(TWO, SIX), dma(SIX), dma(TWO, SIX),
        dma(ngz, TWO), dma(TWO, nz, TWO), dma(FOUR, nz, TWO), dma(FOUR, nz, TWO), dma(FOUR, TWO), dma(FOUR, NY, TWO), dma(FOUR, NY, TWO), dma(THREE, S), dma(THREE, S),
        dma(TWO, TWO, TWO), dma(TWO, TWO, TWO), dma(TWO, TWO, TWO), dma(TWO, TWO, TWO), dma(TWO, TWO, NX), dma(TWO, TWO, NX), dma(TWO, TWO, NX), dma(TWO, TWO, NX), dma(THREE, NX + 1), dma(THREE, NX + 1),
    ]
    anywhere = pl.BlockSpec(memory_space=pl.ANY)
    array = jax.ShapeDtypeStruct
    return pl.pallas_call(
        functools.partial(layers_kernel, tile=tile, nz=nz),
        in_specs=[anywhere] * FOUR,
        out_specs=[anywhere] * 9 + [pl.BlockSpec(memory_space=pltpu.VMEM)],
        out_shape=[
            array(wgu.shape, BF16),
            array(wdn.shape, BF16),
            array((tokens, d), BF16),
            array((d, tokens), BF16),
            array((units, tokens, U), F32),
            array((units, tokens, U), F32),
            array((units, tokens, U), BF16),
            array((TWO * units, NY, ngz, TWO, rz, LANES), BF16),
            array((TWO * units, NY, ngz, rd, cz), BF16),
            array((S, LANES), F32),
        ],
        scratch_shapes=scratch,
        input_output_aliases={TWO: 0, THREE: 1},
        compiler_params=pltpu.CompilerParams(collective_id=1, has_side_effects=True, vmem_limit_bytes=67043328),
        cost_estimate=pl.CostEstimate(flops=15 * TWO * tokens * d * U * units, bytes_accessed=2**28, transcendentals=0),
        name="layers",
    )(x, dy, wgu, wdn)[SIX + 1 :]


def step_kernel(squares, fgu, fd, wg, mg, vg, wu, mu, vu, wd, md, vd, *out, n_units, count):
    ngz, rd, cz = fd.shape[2:]
    fac = jnp.minimum(1.0, 0.5 * lax.rsqrt(squares[0:1] / count + 1e-30))[:, 0:1]

    def adamw(g, w, m, v):
        g = g.astype(F32) * fac
        m = 0.9 * m + 0.1 * g
        v = 0.95 * v + 0.05 * g * g
        step = m * lax.rsqrt(v + 1e-8) + 0.1 * w.astype(F32)
        return (w.astype(F32) - 0.02 * step).astype(BF16), m, v

    rows = wg.shape[1]
    low = lax.broadcasted_iota(jnp.int32, (rows, LANES), 1) < UB
    for h, (w, m, v, outs) in enumerate(((wg, mg, vg, out[0::THREE]), (wu, mu, vu, out[1::THREE]))):
        by_unit = [jnp.concatenate([fgu[j, 0, k, h] for k in range(ngz)], axis=0).astype(F32) for j in range(n_units)]
        for i in range(n_units):
            at = pl.ds(i * LANES, LANES)
            g = jnp.where(low, by_unit[TWO * i % n_units], by_unit[(TWO * i + 1) % n_units])
            outs[0][0, :, at], outs[1][0, :, at], outs[2][0, :, at] = adamw(g, w[0, :, at], m[0, :, at], v[0, :, at])
    outs = out[TWO::THREE]
    for j in range(n_units):
        g = jnp.concatenate([fd[j, 0, k] for k in range(ngz)], axis=1)
        outs[0][0, j, 0], outs[1][0, j, 0], outs[2][0, j, 0] = adamw(g, wd[0, j, 0], md[0, j, 0], vd[0, j, 0])


def optimizer(squares, fgu, fd, weights, m, v):
    layers, rg, ff = weights[0].shape
    n_units = ff // U
    d = weights[2].shape[2]
    _, _, ngz, rd, cz = fd.shape
    rz = rg // ngz
    wide = ff // NY
    down = lambda a: a.reshape(layers, n_units, NY, rd, d)
    col = pl.BlockSpec((1, rg, wide), lambda l, a: (l, 0, a))
    row = pl.BlockSpec((1, n_units, 1, rd, d), lambda l, a: (l, 0, a, 0, 0))
    args = []
    for i in range(3):
        args += [w if i < 2 else down(w) for w in (weights[i], m[i], v[i])]
    shapes = lambda dtype: [jax.ShapeDtypeStruct((layers, rg, ff), dtype)] * 2 + [jax.ShapeDtypeStruct((layers, n_units, NY, rd, d), dtype)]
    out = pl.pallas_call(
        functools.partial(step_kernel, n_units=n_units, count=S * sum(w.size for w in weights)),
        grid=(layers, NY),
        in_specs=[
            pl.BlockSpec((S, LANES), lambda l, a: (0, 0)),
            pl.BlockSpec((n_units, 1, ngz, 2, rz, LANES), lambda l, a: (1 - l, a, 0, 0, 0, 0)),
            pl.BlockSpec((n_units, 1, ngz, rd, cz), lambda l, a: (1 - l, a, 0, 0, 0)),
        ]
        + [col] * 6
        + [row] * 3,
        out_specs=[col, col, row] * 3,
        out_shape=shapes(BF16) + shapes(F32) + shapes(F32),
        name="adamw",
    )(squares, fgu, fd, *args)
    return tuple(o.reshape(layers, -1, d) if i % 3 == 2 else o for i, o in enumerate(out))


def solution(mesh):
    nz = mesh.shape["r"] // NY

    def step(x, dy, *arrays):
        weights, m, v = (arrays[i : i + THREE] for i in (0, THREE, SIX))
        fgu, fd, squares = layers(x[0], dy[0], *prep(*weights), nz)
        return optimizer(squares, fgu, fd, weights, m, v)

    states, cut = P(("rep", "r", "s"), None, None), P(None, "s", None)
    return jax.shard_map(
        step,
        mesh=mesh,
        in_specs=(states, states) + (cut,) * 9,
        out_specs=(P("rep", "s", None),) * 9,
        check_vma=False,
    )
```

```python
import functools

import jax
import jax.numpy as jnp
from jax import lax
from jax.experimental import pallas as pl
from jax.experimental.pallas import tpu as pltpu
from jax.sharding import PartitionSpec as P

NX, NC, NY = 4, 2, 4
S = NX * NC
U = 512
UB = U // S
LANES = 128
TILE = 512
TWO, THREE, FOUR, SIX = 2, 3, 4, 6
BOTH = (0, 1)
F32, BF16 = jnp.float32, jnp.bfloat16
MESH = pl.DeviceIdType.MESH
EPS = 1e-6


def nn(a, b):
    return lax.dot_general(a, b, (((1,), (0,)), ((), ())), preferred_element_type=F32)


def nt(a, b):
    return lax.dot_general(a, b, (((1,), (1,)), ((), ())), preferred_element_type=F32)


def tn(a, b):
    return lax.dot_general(a, b, (((0,), (0,)), ((), ())), preferred_element_type=F32)


def scale_of(wide):
    return lax.rsqrt(jnp.mean(wide * wide, -1, keepdims=True) + EPS)


def other(bit, by):
    return bit + by - TWO * bit * by


def glu_backward(g, u, dh):
    sig = jax.nn.sigmoid(g)
    silu = g * sig
    by_silu = dh * u
    return (silu * u).astype(BF16), (by_silu * (sig + silu * (1.0 - sig))).astype(BF16), (silu * dh).astype(BF16)


class Copy:
    def __init__(self, **what):
        self.what = what

    def __getattr__(self, name):
        return getattr(pltpu.make_async_remote_copy(**self.what), name)


def start(copies):
    for copy in copies:
        copy.start()


def arrived(copies):
    for copy in copies:
        copy.wait_recv()


def sent(copies):
    for copy in copies:
        copy.wait_send()


def done(copies):
    for copy in copies:
        copy.wait()


def prep_kernel(wg, wu, wd, wgu, wdn, block, sem, *, units):
    layers, rows, _ = wg.shape
    s = lax.axis_index("s")
    x, c = lax.div(s, NC), lax.rem(s, NC)
    low = lax.broadcasted_iota(jnp.int32, (rows, LANES), 1) < UB
    copies = []
    for l in range(layers):
        for j in range(units):
            copies.append(pltpu.make_async_copy(wd.at[l, j], wdn.at[l * units + j, x, c], sem.at[1, l, j]))
    start(copies)
    for l in range(layers):
        for j in range(units):
            for h, w in enumerate((wg, wu)):
                for a in range(NX):
                    swap = j % TWO
                    first = (TWO * a + swap) * units + j
                    second = (TWO * a + 1 - swap) * units + j
                    one = w[l, :, pl.ds(first // TWO * LANES, LANES)]
                    two = w[l, :, pl.ds(second // TWO * LANES, LANES)]
                    block[l, j, h, :, pl.ds(a * LANES, LANES)] = jnp.where(low, one, two)
            copy = pltpu.make_async_copy(block.at[l, j], wgu.at[l * units + j, :, x, c], sem.at[0, l, j])
            copy.start()
            copies.append(copy)
    done(copies)


def prep(w_gate, w_up, w_down):
    layers, rows, ff = w_gate.shape
    units, d = ff // U, w_down.shape[-1]
    anywhere = pl.BlockSpec(memory_space=pl.ANY)
    return pl.pallas_call(
        functools.partial(prep_kernel, units=units),
        in_specs=[pl.BlockSpec(memory_space=pltpu.VMEM)] * 3,
        out_specs=[anywhere] * 2,
        out_shape=[jax.ShapeDtypeStruct((layers * units, 2, NX, NC, rows, U), BF16), jax.ShapeDtypeStruct((layers * units, NX, NC, UB, d), BF16)],
        scratch_shapes=[pltpu.VMEM((layers, units, 2, rows, U), BF16), pltpu.SemaphoreType.DMA((2, layers, units))],
        name="prep",
    )(w_gate, w_up, w_down.reshape(layers, units, UB, d))


def layers_kernel(
    x0, dy, wgu_in, wdn_in,
    wgu, wdn, h1, a0T, silu0, slope0, hid0, fgu, fd,
    squares,
    a1, aT, dyv, acc, hid, dgt, dup, wv, wdv, upt,
    ggu, gd, pgu, pd,
    sa1, ra1, sb1, rb1, sa2, ra2, sb2, rb2, res1, res2,
    sa3, ra3, sb3, rb3, sa4, ra4, sb4, rb4, q1, q2,
    zs1, zs2, zr1, zr2, gz1, gz2, ss, sr,
    wsem, asem, tsem, hsem,
    psend, precv, s1s, s1r, s2s, s2r, s3s, s3r, s4s, s4r, zss, zsr, gss, gsr, gls, ys, yr, qss, qsr,
    xas, xar, xbs, xbr, yas, yar, ybs, ybr, dds, ddr,
    *, tile, nz,
):
    tokens, d = dyv.shape
    total_units = wgu.shape[0]
    units = total_units // TWO
    n_tiles = tokens // tile
    ngz = nz - 1

    s, r = lax.axis_index("s"), lax.axis_index("r")
    x, c = lax.div(s, NC), lax.rem(s, NC)
    y, z = lax.div(r, nz), lax.rem(r, nz)
    turn = lambda i, by, n: lax.rem(i + by + n, n)
    x_dev = lambda k: {"s": turn(x, k, NX) * NC + c}
    y_dev = lambda k: {"r": turn(y, k, NY) * nz + z}
    z_dev = lambda k: {"r": y * nz + k}
    partner = {"s": x * NC + 1 - c}
    ways = tuple(enumerate((1, -1)))

    def remote(src, dst, send, recv, dev):
        return Copy(src_ref=src, dst_ref=dst, send_sem=send, recv_sem=recv, device_id=dev, device_id_type=MESH)

    def when(condition, do):
        pl.when(condition)(do)

    barrier = pltpu.get_barrier_semaphore()
    group = [{"s": turn(s, k, S)} for k in range(1, S)]
    peers = group + [y_dev(k) for k in range(1, NY)]
    peers += [z_dev(turn(z, k, nz)) for k in range(1, nz)]
    for dev in peers:
        pl.semaphore_signal(barrier, inc=1, device_id=dev, device_id_type=MESH)
    pl.semaphore_wait(barrier, len(peers))

    def cols(k):
        return pl.ds(pl.multiple_of(k * LANES, LANES), LANES)

    def piece(v, k, q):
        return wgu.at[v, :, k, c, :, cols(q)]

    GU, DOWN = (0,), (1,)

    def x_first(v, which):
        a2 = lax.rem(v, TWO)
        for w, by in ways:
            out = [((piece(v, x, y), wdn.at[v, x, c])[i], i) for i in which]
            yield by, [remote(ref, ref, xas.at[a2, w, i], xar.at[a2, w, i], x_dev(by)) for ref, i in out]

    def x_second(v, which):
        a2 = lax.rem(v, TWO)
        for w, by in ways:
            k = turn(x, -by, NX)
            out = [((wgu.at[v, w, k, c, :, cols(y)], wdn.at[v, k, c, pl.ds(w * (UB // TWO), UB // TWO)])[i], i) for i in which]
            yield by, [remote(ref, ref, xbs.at[a2, w, i], xbr.at[a2, w, i], x_dev(by)) for ref, i in out]

    def y_first(v, which):
        a2 = lax.rem(v, TWO)
        for w, by in ways:
            out = [(piece(v, turn(x, i, NX), y), i) for i in which]
            yield by, [remote(ref, ref, yas.at[a2, w, i], yar.at[a2, w, i], y_dev(by)) for ref, i in out]

    def y_second(v, which):
        a2 = lax.rem(v, TWO)
        for w, by in ways:
            out = [(wgu.at[v, w, turn(x, i, NX), c, :, cols(turn(y, -by, NY))], i) for i in which]
            yield by, [remote(ref, ref, ybs.at[a2, w, i], ybr.at[a2, w, i], y_dev(by)) for ref, i in out]

    def across(v, which):
        a3 = lax.rem(v, THREE)
        out = [(wgu.at[v, :, turn(x, i, NX), c] if i < NX else wdn.at[v, :, c], i) for i in which]
        return [remote(ref, ref, dds.at[a3, i], ddr.at[a3, i], partner) for ref, i in out]

    def every(groups):
        return [copy for _, group in groups for copy in group]

    near, far = (1, NX - 1), (TWO,)
    early = (0, *near, NX)

    def g1(v):
        start(every(x_first(v, GU)))

    def g2(v):
        arrived(every(x_first(v, GU)))
        start(every(x_second(v, GU)))
        start(every(y_first(v, near)))
        start(every(x_first(v, DOWN)))

    def g3(v):
        arrived(every(x_second(v, GU)))
        start(every(y_first(v, far)))
        arrived(every(y_first(v, near)))
        start(every(y_second(v, near)))
        arrived(every(x_first(v, DOWN)))
        start(every(x_second(v, DOWN)))
        sent(every(x_first(v, GU)))

    def g4(v):
        arrived(every(y_first(v, far)))
        start(every(y_second(v, far)))
        arrived(every(y_second(v, near)))
        arrived(every(x_second(v, DOWN)))
        start(across(v, early))
        sent(every(x_first(v, DOWN)))
        sent(every(x_second(v, GU)))
        sent(every(y_first(v, near)))

    def g5(v):
        arrived(every(y_second(v, far)))
        start(across(v, far))
        sent(every(x_second(v, DOWN)))
        sent(every(y_first(v, far)))
        sent(every(y_second(v, near)))

    def g6(v):
        arrived(across(v, early + far))
        sent(across(v, early + far))
        sent(every(y_second(v, far)))
        start(weights(v))

    stages = (g1, g2, g3, g4, g5, g6)

    def gather(*what):
        for number, v in what:
            when(v < total_units, functools.partial(stages[number - 1], v))

    def gather_beside(v, i):
        ahead = (((4, 2),), ((6, 1), (3, 3)), ((2, 4),), ((5, 2), (1, 5)))[i]
        gather(*((number, v + by) for number, by in ahead))

    def weights(v, down_only=False):
        slot, unit = lax.rem(v, TWO), lax.rem(v, total_units)
        swap = lax.rem(lax.rem(unit, units), TWO)
        copies = [] if down_only else [pltpu.make_async_copy(wgu.at[unit, h], wv.at[slot, h], wsem.at[slot, h]) for h in BOTH]
        for q in BOTH:
            copies.append(pltpu.make_async_copy(wdn.at[unit, :, q], wdv.at[slot, :, other(q, swap)], wsem.at[slot, TWO + q]))
        return copies

    class Ring:
        def __init__(self, me, dev, get, put, buffers, send, recv):
            self.me, self.get, self.put = me, get, put
            self.sa, self.ra, self.sb, self.rb = buffers
            self.a = [remote(self.sa(w), self.ra(w), send.at[w], recv.at[w], dev(by)) for w, by in ways]
            at = lambda w, h: TWO + TWO * w + h
            self.b = [[remote(self.sb(w, h), self.rb(w, h), send.at[at(w, h)], recv.at[at(w, h)], dev(by)) for h in BOTH] for w, by in ways]

        def start(self):
            for h in BOTH:
                self.sa(h)[...] = self.get(turn(self.me, TWO, FOUR), h).astype(BF16)
                self.a[h].start()

        def start_near(self):
            for w, by in ways:
                self.sb(w, 1 - w)[...] = self.get(turn(self.me, by, FOUR), 1 - w).astype(BF16)
                self.b[w][1 - w].start()

        def middle(self):
            for h, by in ways:
                self.a[h].wait_recv()
                self.sb(h, h)[...] = (self.get(turn(self.me, by, FOUR), h) + self.ra(h)[...].astype(F32)).astype(BF16)
                self.b[h][h].start()
            sent(self.a)

        def end(self):
            for w in BOTH:
                arrived(self.b[w])
            for h in BOTH:
                self.put(h, self.get(self.me, h) + self.rb(0, h)[...].astype(F32) + self.rb(1, h)[...].astype(F32))
            for w in BOTH:
                sent(self.b[w])

    def slots(u):
        return lax.rem(u, TWO), lax.rem(u, THREE), lax.rem(lax.rem(u, units), TWO)

    def ring1(u):
        a2, p, _ = slots(u)

        def get(k, h):
            return ggu[a2, h, k, c].astype(F32) + pgu[p, h, k].astype(F32)

        def put(h, total):
            for k in range(NY):
                res1[k, h] = total[:, k * LANES : (k + 1) * LANES]

        buffers = lambda h: sa1.at[h], lambda h: ra1.at[a2, h], lambda w, h: sb1.at[a2, w, h], lambda w, h: rb1.at[p, w, h]
        return Ring(x, x_dev, get, put, buffers, s1s.at[a2], s1r.at[p])

    def ring2(u):
        a2, p, swap = slots(u)
        pos = other(c, swap)

        def get(k, h):
            return gd[a2, pl.ds(TWO * h, TWO), pos, k].astype(F32) + pd[p, pl.ds(TWO * h, TWO), k].astype(F32)

        def put(h, total):
            res2[pl.ds(TWO * h, TWO)] = total

        buffers = lambda h: sa2.at[h], lambda h: ra2.at[a2, h], lambda w, h: sb2.at[a2, w, h], lambda w, h: rb2.at[p, w, h]
        return Ring(y, y_dev, get, put, buffers, s2s.at[a2], s2r.at[p])

    def ring3(u):
        a2, _, _ = slots(u)

        def get(k, h):
            return res1[k, h]

        def put(h, total):
            rows = total.shape[0] // ngz
            for k in range(ngz):
                q1[k, h] = total[k * rows : (k + 1) * rows]

        buffers = lambda h: sa3.at[h], lambda h: ra3.at[a2, h], lambda w, h: sb3.at[w, h], lambda w, h: rb3.at[a2, w, h]
        return Ring(y, y_dev, get, put, buffers, s3s, s3r.at[a2])

    cut = [pl.ds(0, U), pl.ds(U, d - U)]

    def ring4(u):
        a2, _, _ = slots(u)

        def get(k, h):
            return res2[k, :, cut[h]]

        def put(h, total):
            q2[:, cut[h]] = total

        buffers = lambda h: sa4.at[:, cut[h]], lambda h: ra4.at[a2, :, cut[h]], lambda w, h: sb4.at[w, :, cut[h]], lambda w, h: rb4.at[a2, w, :, cut[h]]
        return Ring(x, x_dev, get, put, buffers, s4s, s4r.at[a2])

    def to_partner(u):
        a2, p, swap = slots(u)
        ends = [(ggu.at[a2, h, :, 1 - c], pgu.at[p, h]) for h in BOTH] + [(gd.at[a2, :, other(1 - c, swap)], pd.at[p])]
        return [remote(src, dst, psend.at[i], precv.at[p, i], partner) for i, (src, dst) in enumerate(ends)]

    def c1(u):
        copies = to_partner(u)
        arrived(copies[:TWO])
        ring1(u).start()
        arrived(copies[TWO:])
        ring2(u).start()
        sent(copies)

    def c1b(u):
        ring1(u).start_near()
        ring2(u).start_near()

    def c2(u):
        ring1(u).middle()
        ring2(u).middle()

    def c3(u):
        ring1(u).end()
        ring3(u).start()
        ring3(u).start_near()
        ring2(u).end()
        ring4(u).start()
        ring4(u).start_near()

    def c4(u):
        ring3(u).middle()
        ring4(u).middle()

    def others(n, do):
        def one(k, _):
            when(k != z, functools.partial(do, k))
            return 0

        lax.fori_loop(0, n, one, 0)

    def z_copies(u, k, sender=None):
        a2 = lax.rem(u, TWO)
        sender = z if sender is None else sender
        ends = (zs1.at[k], zr1.at[a2, sender]), (zs2.at[k], zr2.at[a2, sender])
        return [remote(src, dst, zss.at[k, i], zsr.at[a2, sender, i], z_dev(k)) for i, (src, dst) in enumerate(ends)]

    def c5(u):
        ring3(u).end()
        ring4(u).end()
        width = d // ngz
        for k in range(ngz):
            zs1[k] = q1[k].astype(BF16)
            zs2[k] = q2[:, pl.ds(k * width, width)].astype(BF16)
        others(ngz, lambda k: start(z_copies(u, k)))

    def gather_copies(u, k, sender=None):
        a2 = lax.rem(u, TWO)
        sender = z if sender is None else sender
        ends = (gz1.at[a2], fgu.at[u, y, sender]), (gz2.at[a2], fd.at[u, y, sender])
        return [remote(src, dst, gss.at[a2, k, i], gsr.at[a2, sender, i], z_dev(k)) for i, (src, dst) in enumerate(ends)]

    def own_copies(u):
        a2 = lax.rem(u, TWO)
        ends = (gz1.at[a2], fgu.at[u, y, z]), (gz2.at[a2], fd.at[u, y, z])
        return [pltpu.make_async_copy(src, dst, gls.at[a2, i]) for i, (src, dst) in enumerate(ends)]

    def c6(u):
        a2 = lax.rem(u, TWO)

        def sums():
            others(nz, lambda k: arrived(z_copies(u, 0, k)))
            zone, width = lax.rem(z, ngz), d // ngz
            one, two = q1[zone], q2[:, pl.ds(pl.multiple_of(zone * width, LANES), width)]
            for k in range(nz):
                one += jnp.where(k == z, 0.0, zr1[a2, k].astype(F32))
                two += jnp.where(k == z, 0.0, zr2[a2, k].astype(F32))
            one, two = one.astype(BF16), two.astype(BF16)
            gz1[a2], gz2[a2] = one, two
            one, two = one.astype(F32), two.astype(F32)
            ss[...] += jnp.full(ss.shape, jnp.sum(one * one) + jnp.sum(two * two))
            start(own_copies(u))
            others(nz, lambda k: start(gather_copies(u, k)))

        when(z < ngz, sums)
        others(ngz, lambda k: sent(z_copies(u, k)))

    def y_copies(u):
        a4 = lax.rem(u, FOUR)
        ends = fgu.at[u, y], fd.at[u, y]
        return [remote(ref, ref, ys.at[a4, by - 1, i], yr.at[a4, by - 1, i], y_dev(by)) for by in range(1, NY) for i, ref in enumerate(ends)]

    def c7(u):
        others(ngz, lambda k: arrived(gather_copies(u, 0, k)))

        def mine():
            done(own_copies(u))
            others(nz, lambda k: sent(gather_copies(u, k)))

        when(z < ngz, mine)
        start(y_copies(u))

    def c8(u):
        arrived(y_copies(u))
        sent(y_copies(u))

    plan = {1: ((c8, 5), (c5, 3), (c1, 1)), 2: ((c3, 2), (c7, 4)), 3: ((c1b, 1),), 4: ((c4, 2), (c6, 3), (c2, 1))}

    def steps(t, place):
        for step, behind in plan.get(place, ()):
            u = t - behind
            when((u >= 0) & (u < total_units), functools.partial(step, u))

    def rows_of(i):
        return pl.ds(i * tile if isinstance(i, int) else pl.multiple_of(i * tile, tile), tile)

    def weight_gradients(t):
        a2 = lax.rem(t, TWO)
        copies = to_partner(t)
        for h, by in enumerate((dgt, dup)):
            ggu[a2, h] = nn(aT[...], by[...]).astype(BF16).reshape(ggu.shape[TWO:])
            copies[h].start()
            steps(t, THREE + h)
        gd[a2] = tn(hid[...], dyv[...]).astype(BF16).reshape(gd.shape[1:])
        copies[TWO].start()

    load = pltpu.make_async_copy(x0, dyv, asem.at[0])
    load.start()
    g1(0)
    ss[...] = jnp.zeros(ss.shape, F32)
    load.wait()
    keep = pltpu.make_async_copy(aT, a0T, asem.at[1])

    def norm(i, _):
        rows = rows_of(i)
        wide = dyv[rows].astype(F32)
        wide = wide * scale_of(wide)
        a1[rows] = wide.astype(BF16)
        aT[:, rows] = wide.T.astype(BF16)
        acc[0, rows] = jnp.zeros((tile, d), F32)
        return 0

    lax.fori_loop(0, n_tiles, norm, 0)
    keep.start()

    for number, v in (
        (2, 0), (1, 1), (3, 0), (4, 0), (2, 1), (5, 0), (3, 1), (1, 2), (6, 0), (4, 1), (2, 2), (1, 3), (5, 1), (3, 2), (2, 3), (1, 4),
    ):
        if v < total_units:
            stages[number - 1](v)

    def out_tile(j, i):
        slot = i % TWO
        at, rows = pl.ds(slot * tile, tile), pl.ds(i * tile, tile)
        return [
            pltpu.make_async_copy(acc.at[1, at, pl.ds(0, U)], silu0.at[j, rows], tsem.at[slot, 0]),
            pltpu.make_async_copy(upt.at[at], slope0.at[j, rows], tsem.at[slot, 1]),
        ]

    def out_hidden(j, i):
        rows = pl.ds(i * tile, tile)
        return [pltpu.make_async_copy(hid.at[rows], hid0.at[j, rows], hsem.at[i])]

    def forward(j, _):
        slot = lax.rem(j, TWO)
        done(weights(j))
        w_g, w_u, w_d = wv[slot, 0].reshape(d, U), wv[slot, 1].reshape(d, U), wdv[slot].reshape(U, d)
        for i in range(n_tiles):
            rows = pl.ds(i * tile, tile)
            at = pl.ds(i % TWO * tile, tile)
            if i < TWO:
                when(j > 0, lambda: done(out_tile(j, i)))
            else:
                done(out_tile(j, i))
            when(j > 0, lambda: done(out_hidden(j, i)))
            g, u = nn(a1[rows], w_g), nn(a1[rows], w_u)
            sig = jax.nn.sigmoid(g)
            silu = g * sig
            acc[1, at, pl.ds(0, U)], upt[at] = silu, u * (sig + silu * (1.0 - sig))
            one = (silu * u).astype(BF16)
            hid[rows] = one
            acc[0, rows] += nn(one, w_d)
            start(out_tile(j, i) + out_hidden(j, i))
            gather_beside(j, i)
        return 0

    lax.fori_loop(0, units, forward, 0)
    for i in range(min(TWO, n_tiles)):
        done(out_tile(0, i))
    for i in range(n_tiles):
        done(out_hidden(0, i))
    keep.wait()

    def between(i, _):
        rows = rows_of(i)
        h = dyv[rows] + acc[0, rows].astype(BF16)
        hid[rows], dgt[rows, cut_low] = h[:, :U], h[:, U:]
        pltpu.make_async_copy(dy.at[rows], dyv.at[rows], asem.at[0]).start()
        wide = h.astype(F32)
        wide = wide * scale_of(wide)
        a1[rows] = wide.astype(BF16)
        aT[:, rows] = wide.T.astype(BF16)
        for h in BOTH:
            acc[h, rows] = jnp.zeros((tile, d), F32)
        return 0

    cut_low = pl.ds(0, d - U)
    lax.fori_loop(0, n_tiles, between, 0)
    keep = [pltpu.make_async_copy(hid, h1.at[:, cut[0]], asem.at[1]), pltpu.make_async_copy(dgt.at[:, cut_low], h1.at[:, cut[1]], asem.at[TWO])]
    start(keep)
    pltpu.make_async_copy(dy, dyv, asem.at[0]).wait()
    done(keep)

    def both_passes(t, _):
        v = t + units
        slot = lax.rem(v, TWO)
        steps(t, 0)
        when(t == units - 1, lambda: start(weights(total_units, True)))
        done(weights(v))
        w_g, w_u, w_d = wv[slot, 0].reshape(d, U), wv[slot, 1].reshape(d, U), wdv[slot].reshape(U, d)
        for i in range(n_tiles):
            rows = pl.ds(i * tile, tile)
            g, u = nn(a1[rows], w_g), nn(a1[rows], w_u)
            dh = nt(dyv[rows], w_d).astype(BF16).astype(F32)
            hid[rows], by_gate, by_up = glu_backward(g, u, dh)
            dgt[rows], dup[rows] = by_gate, by_up
            acc[0, rows] += nt(by_up, w_u)
            acc[1, rows] += nt(by_gate, w_g)
            gather_beside(v, i)
            if i == 1:
                steps(t, 1)
        when(t == units - 1, loads[0].start)
        steps(t, TWO)
        weight_gradients(t)
        return 0

    loads = [pltpu.make_async_copy(h1, a1, asem.at[0]), pltpu.make_async_copy(a0T, aT, asem.at[1])]
    lax.fori_loop(0, units, both_passes, 0)

    def in_tile(j, i):
        rows = rows_of(i)
        ends = (silu0, 0), (slope0, 1)
        return [pltpu.make_async_copy(src.at[j, rows], acc.at[h, rows, pl.ds(0, U)], tsem.at[TWO + i, h]) for src, h in ends]

    loads[1].start()
    loads[0].wait()

    def cotangent(i, _):
        rows = rows_of(i)
        wide = a1[rows].astype(F32)
        scale = scale_of(wide)
        by_a = (acc[0, rows].astype(BF16).astype(F32) + acc[1, rows].astype(BF16).astype(F32)).astype(BF16).astype(F32)
        inner = jnp.sum(wide * by_a, -1, keepdims=True)
        by_h = by_a * scale - wide * (inner * (scale * scale * scale) * (1.0 / d))
        dyv[rows] = (dyv[rows].astype(F32) + by_h.astype(BF16).astype(F32)).astype(BF16)
        start(in_tile(0, i))
        return 0

    lax.fori_loop(0, n_tiles, cotangent, 0)

    def backward_only(t, _):
        j = t - units
        v = t + units
        slot = lax.rem(v, TWO)
        hidden = pltpu.make_async_copy(hid0.at[j], hid, hsem.at[0])
        hidden.start()
        steps(t, 0)
        when(j < units - 1, lambda: start(weights(v + 1, True)))
        done(weights(v, True))
        w_d = wdv[slot].reshape(U, d)
        for i in range(n_tiles):
            rows = pl.ds(i * tile, tile)
            done(in_tile(j, i))
            dh = nt(dyv[rows], w_d).astype(BF16).astype(F32)
            dup[rows] = (acc[0, rows, pl.ds(0, U)] * dh).astype(BF16)
            dgt[rows] = (acc[1, rows, pl.ds(0, U)] * dh).astype(BF16)
            if i == 1:
                steps(t, 1)
        steps(t, TWO)

        def ahead():
            for i in range(n_tiles):
                start(in_tile(j + 1, i))

        when(j < units - 1, ahead)
        hidden.wait()
        when(j == 0, loads[1].wait)
        weight_gradients(t)
        return 0

    lax.fori_loop(units, total_units, backward_only, 0)

    last = total_units - 1
    for do, before in (
        (c5, 2), (c3, 1), (c7, 3), (c8, 4), (c1, 0), (c1b, 0), (c4, 1), (c6, 2), (c2, 0), (c5, 1), (c7, 2), (c3, 0), (c6, 1), (c4, 0), (c8, 3), (c5, 0), (c6, 0),
    ):
        if before <= last:
            do(last - before)

    def exchange(number, devs):
        copies = [remote(ss, sr.at[number, i], qss.at[number, i], qsr.at[number, i], dev) for i, dev in enumerate(devs)]
        start(copies)

        def finish():
            arrived(copies)
            sent(copies)
            total = ss[...]
            for i in range(len(devs)):
                total += sr[number, i]
            ss[...] = total

        return finish

    rings = [z_dev(turn(z, k, nz)) for k in range(1, nz)], [y_dev(k) for k in range(1, NY)], group
    rest = ((c7, 1), (c8, 2)), ((c7, 0),), ((c8, 1), (c8, 0))
    for number, devs in enumerate(rings):
        finish = exchange(number, devs)
        for do, before in rest[number]:
            if before <= last:
                do(last - before)
        finish()
    squares[...] = ss[...]


def layers(x, dy, wgu, wdn, nz):
    tokens, d = x.shape
    units = wgu.shape[0] // TWO
    tile = TILE
    n_tiles = tokens // tile
    rg, ngz = d // S, nz - 1
    rz, cz, rd = rg // ngz, d // ngz, UB // NY
    vmem = lambda *shape, dtype=BF16: pltpu.VMEM(shape, dtype)
    slots = lambda *shape: [vmem(*lead, *shape) for lead in ((TWO,), (TWO, TWO), (TWO, TWO, TWO), (THREE, TWO, TWO))]
    small = lambda *shape: [vmem(*lead, *shape) for lead in ((TWO,), (TWO, TWO), (TWO, TWO), (TWO, TWO, TWO))]
    narrow = lambda *shape: [vmem(*lead, *shape) for lead in ((), (TWO,), (TWO,), (TWO, TWO))]
    dma = lambda *shape: pltpu.SemaphoreType.DMA(shape)
    scratch = [
        vmem(tokens, d), vmem(d, tokens), vmem(tokens, d), vmem(TWO, tokens, d, dtype=F32),
        vmem(tokens, U), vmem(tokens, U), vmem(tokens, U),
        vmem(TWO, TWO, NX, NC, rg, U), vmem(TWO, NX, NC, UB, d), vmem(min(TWO, n_tiles) * tile, U, dtype=F32),
        vmem(TWO, TWO, NX, NC, rg, U), vmem(TWO, NX, NC, NY, rd, d), vmem(THREE, TWO, NX, rg, U), vmem(THREE, NX, NY, rd, d),
        *slots(rg, U), *slots(TWO, rd, d),
        vmem(NY, TWO, rg, LANES, dtype=F32), vmem(NX, rd, d, dtype=F32),
        *small(rg, LANES), *narrow(rd, d),
        vmem(ngz, TWO, rz, LANES, dtype=F32), vmem(rd, d, dtype=F32),
        vmem(ngz, TWO, rz, LANES), vmem(ngz, rd, cz), vmem(TWO, nz, TWO, rz, LANES), vmem(TWO, nz, rd, cz),
        vmem(TWO, TWO, rz, LANES), vmem(TWO, rd, cz), vmem(S, LANES, dtype=F32), vmem(THREE, S, S, LANES, dtype=F32),
        dma(TWO, FOUR), dma(THREE), dma(TWO + n_tiles, TWO), dma(n_tiles),
        dma(THREE), dma(THREE, THREE), dma(TWO, SIX), dma(THREE, SIX), dma(TWO, SIX), dma(THREE, SIX), dma(SIX), dma(TWO, SIX), dma(SIX), dma(TWO, SIX),
        dma(ngz, TWO), dma(TWO, nz, TWO), dma(TWO, nz, TWO), dma(TWO, nz, TWO), dma(TWO, TWO), dma(FOUR, NY - 1, TWO), dma(FOUR, NY - 1, TWO), dma(THREE, S), dma(THREE, S),
        dma(TWO, TWO, TWO), dma(TWO, TWO, TWO), dma(TWO, TWO, TWO), dma(TWO, TWO, TWO), dma(TWO, TWO, NX), dma(TWO, TWO, NX), dma(TWO, TWO, NX), dma(TWO, TWO, NX), dma(THREE, NX + 1), dma(THREE, NX + 1),
    ]
    anywhere = pl.BlockSpec(memory_space=pl.ANY)
    array = jax.ShapeDtypeStruct
    return pl.pallas_call(
        functools.partial(layers_kernel, tile=tile, nz=nz),
        in_specs=[anywhere] * FOUR,
        out_specs=[anywhere] * 9 + [pl.BlockSpec(memory_space=pltpu.VMEM)],
        out_shape=[
            array(wgu.shape, BF16),
            array(wdn.shape, BF16),
            array((tokens, d), BF16),
            array((d, tokens), BF16),
            array((units, tokens, U), F32),
            array((units, tokens, U), F32),
            array((units, tokens, U), BF16),
            array((TWO * units, NY, ngz, TWO, rz, LANES), BF16),
            array((TWO * units, NY, ngz, rd, cz), BF16),
            array((S, LANES), F32),
        ],
        scratch_shapes=scratch,
        input_output_aliases={TWO: 0, THREE: 1},
        compiler_params=pltpu.CompilerParams(collective_id=1, has_side_effects=True, vmem_limit_bytes=67043328),
        cost_estimate=pl.CostEstimate(flops=15 * TWO * tokens * d * U * units, bytes_accessed=2**28, transcendentals=0),
        name="layers",
    )(x, dy, wgu, wdn)[SIX + 1 :]


def step_kernel(squares, fgu, fd, wg, mg, vg, wu, mu, vu, wd, md, vd, *out, n_units, count):
    ngz, rd, cz = fd.shape[2:]
    fac = jnp.minimum(1.0, 0.5 * lax.rsqrt(squares[0:1] / count + 1e-30))[:, 0:1]

    def adamw(g, w, m, v):
        g = g.astype(F32) * fac
        m = 0.9 * m + 0.1 * g
        v = 0.95 * v + 0.05 * g * g
        step = m * lax.rsqrt(v + 1e-8) + 0.1 * w.astype(F32)
        return (w.astype(F32) - 0.02 * step).astype(BF16), m, v

    rows = wg.shape[1]
    low = lax.broadcasted_iota(jnp.int32, (rows, LANES), 1) < UB
    for h, (w, m, v, outs) in enumerate(((wg, mg, vg, out[0::THREE]), (wu, mu, vu, out[1::THREE]))):
        by_unit = [jnp.concatenate([fgu[j, 0, k, h] for k in range(ngz)], axis=0).astype(F32) for j in range(n_units)]
        for i in range(n_units):
            at = pl.ds(i * LANES, LANES)
            g = jnp.where(low, by_unit[TWO * i % n_units], by_unit[(TWO * i + 1) % n_units])
            outs[0][0, :, at], outs[1][0, :, at], outs[2][0, :, at] = adamw(g, w[0, :, at], m[0, :, at], v[0, :, at])
    outs = out[TWO::THREE]
    for j in range(n_units):
        g = jnp.concatenate([fd[j, 0, k] for k in range(ngz)], axis=1)
        outs[0][0, j, 0], outs[1][0, j, 0], outs[2][0, j, 0] = adamw(g, wd[0, j, 0], md[0, j, 0], vd[0, j, 0])


def optimizer(squares, fgu, fd, weights, m, v):
    layers, rg, ff = weights[0].shape
    n_units = ff // U
    d = weights[2].shape[2]
    _, _, ngz, rd, cz = fd.shape
    rz = rg // ngz
    wide = ff // NY
    down = lambda a: a.reshape(layers, n_units, NY, rd, d)
    col = pl.BlockSpec((1, rg, wide), lambda l, a: (l, 0, a))
    row = pl.BlockSpec((1, n_units, 1, rd, d), lambda l, a: (l, 0, a, 0, 0))
    args = []
    for i in range(3):
        args += [w if i < 2 else down(w) for w in (weights[i], m[i], v[i])]
    shapes = lambda dtype: [jax.ShapeDtypeStruct((layers, rg, ff), dtype)] * 2 + [jax.ShapeDtypeStruct((layers, n_units, NY, rd, d), dtype)]
    out = pl.pallas_call(
        functools.partial(step_kernel, n_units=n_units, count=S * sum(w.size for w in weights)),
        grid=(layers, NY),
        in_specs=[
            pl.BlockSpec((S, LANES), lambda l, a: (0, 0)),
            pl.BlockSpec((n_units, 1, ngz, 2, rz, LANES), lambda l, a: (1 - l, a, 0, 0, 0, 0)),
            pl.BlockSpec((n_units, 1, ngz, rd, cz), lambda l, a: (1 - l, a, 0, 0, 0)),
        ]
        + [col] * 6
        + [row] * 3,
        out_specs=[col, col, row] * 3,
        out_shape=shapes(BF16) + shapes(F32) + shapes(F32),
        name="adamw",
    )(squares, fgu, fd, *args)
    return tuple(o.reshape(layers, -1, d) if i % 3 == 2 else o for i, o in enumerate(out))


def solution(mesh):
    nz = mesh.shape["r"] // NY

    def step(x, dy, *arrays):
        weights, m, v = (arrays[i : i + THREE] for i in (0, THREE, SIX))
        fgu, fd, squares = layers(x[0], dy[0], *prep(*weights), nz)
        return optimizer(squares, fgu, fd, weights, m, v)

    states, cut = P(("rep", "r", "s"), None, None), P(None, "s", None)
    return jax.shard_map(
        step,
        mesh=mesh,
        in_specs=(states, states) + (cut,) * 9,
        out_specs=(P("rep", "s", None),) * 9,
        check_vma=False,
    )
```
